256 devices in a mesh: group: 2 (over y), temp: 4 (over x), gz: 32 (over z, core).
Axes of the slice: x: 4, y: 2, z: 16, core: 2. Of those that a mesh axis runs over, the one named last changes fastest.
The devices are a block of a 4x16x16 slice.
Arguments:
- spin_state: float32 [16, 3, 128, 128, 128], P(('group', 'temp'), None, 'gz'), parts along dimension 0, may hold values from -1 to 1, as said below
- couplings: float32 [3, 256, 128, 128], P(None, ('group', 'gz')), parts along dimension 1, may hold values from -12 to 12
- inverse_temps: float32 [16], P(('group', 'temp')), parts along dimension 0, may hold values from 0.3 to 3
- colour_order: int32 [16], P(('group', 'temp')), parts along dimension 0, may hold values 0 or 1
- heat_level: float32 [16, 128, 128, 128], P(('group', 'temp'), 'gz'), parts along dimension 0, may hold values from 0.001 to 0.999
- heat_height: float32 [16, 128, 128, 128], P(('group', 'temp'), 'gz'), parts along dimension 0, may hold values from -1 to 1
- heat_angle: float32 [16, 128, 128, 128], P(('group', 'temp'), 'gz'), parts along dimension 0, may hold values from -3.140625 to 3.140625
- swap_bits: int32 [16], P(('group', 'temp')), parts along dimension 0, may hold values 0 or 1
Outputs:
- spin_final: float32 [16, 3, 128, 128, 128], P(('group', 'temp'), None, 'gz'), parts along dimension 0
- energies: float32 [16], P(('group', 'temp')), parts along dimension 0
The draws below stay inside these ranges and needn't reach their ends.
There are 2 independent parts, one for each index of `group`. The reference program is written for one: setup_inputs(seed, part) draws one part's arguments, and reference() takes and returns one part's arrays. A program takes and returns all parts, laid end to end along the dimension named above; each array names one. Nothing has to cross between parts.
Inputs may be any that keep to these rules, and one draw needn't show every extreme that they name: `spin_state`: every site's three components form a vector of unit length.
All inputs are finite; a program needn't handle non-finite values. No bound on the sum of `colour_order` or of `swap_bits` on one device may be relied on, other than what follows from the above.
Results may differ from the reference program's by a relative error of at most 0.0003.
Values sent between devices are 32-bit elements; how exact they have to be, the bound alone decides.
No kernel may reach another device: no remote copies, remote signals or barrier semaphores. Data moves between devices by JAX's collectives and lax.ppermute only.
A program may use at most 64 MiB of HBM per device.

```python
import math
import jax
import jax.numpy as jnp
from jax import lax

LX = 128
LY = 128
OR_SWEEPS = 2
REPLICAS = 8
NZ = 128


def draw_spin_state(key, part):
    first_key, second_key = jax.random.split(jax.random.fold_in(key, 11))
    array_shape = (REPLICAS, NZ, LY, LX)
    height = jax.random.uniform(first_key, array_shape, jnp.float32, -1.0, 1.0)
    azimuth = jax.random.uniform(second_key, array_shape, jnp.float32, -math.pi, math.pi)
    side = jnp.sqrt(jnp.maximum(1.0 - height * height, 0.0))
    return jnp.stack([side * jnp.cos(azimuth), side * jnp.sin(azimuth), height], axis=1)


def draw_couplings(key, part):
    first_key = jax.random.fold_in(key, 23)
    array_shape = (3, NZ, LY, LX)
    position = jnp.arange(NZ, dtype=jnp.float32) / max(NZ - 1, 1)
    values = jnp.clip(jax.random.normal(first_key, array_shape, jnp.float32), -4.0, 4.0)
    factor = 1.0 + 2.0 * position
    return values * factor[None, :, None, None]


def place_ends(array, rng, smallest, largest):
    longest = array.shape.index(max(array.shape))
    spots = []
    for shift in (0, 1):
        where = [jax.random.randint(jax.random.fold_in(rng, axis), (), 0, length) for axis, length in enumerate(array.shape)]
        where[longest] = (where[longest] + shift) % array.shape[longest]
        spots.append(tuple(where))
    return array.at[spots[0]].set(smallest).at[spots[1]].set(largest)


def steps_of(rng, dims, shards, low, largest):
    level = 1.0
    for dim, blocks in shards:
        draws = jax.random.uniform(jax.random.fold_in(jax.random.fold_in(rng, 6), dim), (blocks,), jnp.float32, low / len(shards), largest / len(shards))
        level = level * jnp.repeat(jnp.exp(draws), dims[dim] // blocks).reshape((-1,) + (1,) * (len(dims) - 1 - dim))
    return level


def setup_inputs(seed: int = 0, part: int = 0) -> dict:
    streams_of = jax.random.split(jax.random.key(seed), 9)
    part_splits = jax.random.split(jax.random.fold_in(streams_of[8], part), 9)
    return {
        "spin_state": draw_spin_state(jax.random.fold_in(jax.random.fold_in(streams_of[8], part), 71), part),
        "couplings": draw_couplings(jax.random.fold_in(jax.random.fold_in(streams_of[8], part), 71), part),
        "inverse_temps": jnp.clip(jnp.exp(math.log(3.0) - 2.3025851 * jax.random.uniform(part_splits[2], (REPLICAS,), jnp.float32) ** steps_of(part_splits[2], (REPLICAS,), ((0, 4),), -0.2, 0.2)), 0.3, 3.0),
        "colour_order": place_ends((jax.random.randint(part_splits[3], (REPLICAS,), 0, 2) < 1).astype(jnp.int32), jax.random.fold_in(part_splits[3], 1), 0, 1),
        "heat_level": jnp.clip(0.001 + 0.998 * jax.random.uniform(part_splits[4], (REPLICAS, NZ, LY, LX), jnp.float32) ** steps_of(part_splits[4], (REPLICAS, NZ, LY, LX), ((0, 4), (1, 32)), -0.2, 0.2), 0.001, 0.999),
        "heat_height": jnp.clip(jax.random.uniform(part_splits[5], (REPLICAS, NZ, LY, LX), jnp.float32, -1.0, 1.0) * steps_of(part_splits[5], (REPLICAS, NZ, LY, LX), ((0, 4), (1, 32)), -0.4, 0.0), -1.0, 1.0),
        "heat_angle": jnp.clip(jax.random.uniform(part_splits[6], (REPLICAS, NZ, LY, LX), jnp.float32, -3.140625, 3.140625), -3.140625, 3.140625),
        "swap_bits": place_ends((jax.random.randint(part_splits[7], (REPLICAS,), 0, 4) < 3).astype(jnp.int32), jax.random.fold_in(part_splits[7], 1), 0, 1),
    }


def neighbour_sum(current, bonds):
    east_bond, north_bond, upper_bond = (bonds[0], bonds[1], bonds[2])
    summed = east_bond * jnp.roll(current, -1, 3) + jnp.roll(east_bond, 1, 2) * jnp.roll(current, 1, 3)
    summed = summed + north_bond * jnp.roll(current, -1, 2) + jnp.roll(north_bond, 1, 1) * jnp.roll(current, 1, 2)
    summed = summed + upper_bond * jnp.roll(current, -1, 1) + jnp.roll(upper_bond, 1, 0) * jnp.roll(current, 1, 1)
    return summed

def reflect(current, pulled, component_axis):
    projection = lax.optimization_barrier(jnp.sum(current * pulled, axis=component_axis, keepdims=True))
    square = lax.optimization_barrier(jnp.sum(pulled * pulled, axis=component_axis, keepdims=True))
    return 2.0 * projection / jnp.maximum(square, 0.01) * pulled - current

def heat_bath(pulled, beta_value, uniform_level, cosine_draw, angle_draw, component_axis):
    square = lax.optimization_barrier(jnp.sum(pulled * pulled, axis=component_axis, keepdims=True))
    strength = jnp.sqrt(jnp.maximum(square, 0.01))
    unit_axis = pulled / strength
    reach = beta_value * strength
    cosine = 1.0 + jnp.log1p(uniform_level * jnp.expm1(-2.0 * reach)) / reach
    side = jnp.sqrt(jnp.maximum(1.0 - cosine_draw * cosine_draw, 0.0))
    proposal = jnp.concatenate([side * jnp.cos(angle_draw), side * jnp.sin(angle_draw), cosine_draw], axis=component_axis)
    along_axis = lax.optimization_barrier(jnp.sum(proposal * unit_axis, axis=component_axis, keepdims=True))
    tangent = proposal - along_axis * unit_axis
    tangent = tangent / jnp.sqrt(jnp.maximum(lax.optimization_barrier(jnp.sum(tangent * tangent, axis=component_axis, keepdims=True)), 0.0001))
    return cosine * unit_axis + jnp.sqrt(jnp.maximum(1.0 - cosine * cosine, 0.0)) * tangent

def pair_swap(stacked, decisions):
    flipped = stacked[:, ::-1]
    taking = (decisions != 0).reshape((-1,) + (1,) * (stacked.ndim - 1))
    return jnp.where(taking, flipped, stacked)

def reference(spin_state, couplings, inverse_temps, colour_order, heat_level, heat_height, heat_angle, swap_bits):
    plane_index = jnp.arange(NZ, dtype=jnp.int32)
    row_index = jnp.arange(LY, dtype=jnp.int32)
    column_index = jnp.arange(LX, dtype=jnp.int32)
    site_sum = plane_index[:, None, None] + row_index[None, :, None] + column_index[None, None, :]

    def one_replica(packed):
        current, beta_value, start_colour, uniform_level, cosine_draw, angle_draw = packed
        parity = (site_sum + start_colour) % 2
        colours = ((parity == 0)[None], (parity == 1)[None])
        for sweep_index in range(OR_SWEEPS):
            for chosen in colours:
                pulled = neighbour_sum(current, couplings)
                current = jnp.where(chosen, reflect(current, pulled, 0), current)
        for chosen in colours:
            pulled = neighbour_sum(current, couplings)
            renewed = heat_bath(pulled, beta_value, uniform_level[None], cosine_draw[None], angle_draw[None], 0)
            current = jnp.where(chosen, renewed, current)
        bond_sum = couplings[0] * jnp.roll(current, -1, 3) + couplings[1] * jnp.roll(current, -1, 2) + couplings[2] * jnp.roll(current, -1, 1)
        energy = -jnp.sum(current * bond_sum) / (LX * LY * NZ)
        return (current, energy)
    swept, energy_all = lax.map(one_replica, (spin_state, inverse_temps, colour_order, heat_level, heat_height, heat_angle))
    count = REPLICAS
    tail_shape = swept.shape[1:]
    swept = pair_swap(swept.reshape((count // 2, 2) + tail_shape), swap_bits[0::2]).reshape(swept.shape)
    energy_all = pair_swap(energy_all.reshape((count // 2, 2)), swap_bits[0::2]).reshape((count,))
    middle = pair_swap(swept[1:count - 1].reshape(((count - 2) // 2, 2) + tail_shape), swap_bits[1:count - 1:2])
    swept = jnp.concatenate([swept[:1], middle.reshape((count - 2,) + tail_shape), swept[count - 1:]], axis=0)
    middle_energy = pair_swap(energy_all[1:count - 1].reshape(((count - 2) // 2, 2)), swap_bits[1:count - 1:2])
    energy_all = jnp.concatenate([energy_all[:1], middle_energy.reshape((count - 2,)), energy_all[count - 1:]], axis=0)
    return (swept, energy_all)
```

```python
import functools

import jax
import jax.numpy as jnp
from jax import lax
from jax.experimental import pallas as pl
from jax.experimental.pallas import tpu as pltpu
from jax.sharding import PartitionSpec as P

F32 = jnp.float32


def kernel_call(body, name, outs, in_specs, mib=24, out_specs=None):
    return pl.pallas_call(
        body,
        name=name,
        out_shape=outs,
        in_specs=in_specs,
        out_specs=out_specs if out_specs is not None else [VM] * len(outs),
        compiler_params=pltpu.CompilerParams(vmem_limit_bytes=mib * 1024 * 1024),
    )


VM = pl.BlockSpec(memory_space=pltpu.VMEM)
SM = pl.BlockSpec(memory_space=pltpu.SMEM)


def vm(*shape):
    return pltpu.VMEM(shape, F32)


def core_index():
    return lax.rem(lax.axis_index("gz"), 2)


def slot_replica(swap, slot):
    bit = (swap[0] != 0).astype(jnp.int32)
    return bit if slot == 0 else 1 - bit


def lane_even(rows, columns, offset):
    lane = lax.broadcasted_iota(jnp.int32, (rows, columns), 1)
    return ((lane + offset) & 1) == 0


def folded(ref, index, half):
    even = ref[(*index, pl.ds(0, half, stride=2), slice(None))]
    odd = ref[(*index, pl.ds(1, half, stride=2), slice(None))]
    return even, odd


def load_kernel(planes, half, swap, colour, spin, sx0, sx1, si0, si1, am0, am1):
    core = core_index()
    columns = spin.shape[-1]
    for slot, sx, si, am in ((0, sx0, si0, am0), (1, sx1, si1, am1)):
        rep = slot_replica(swap, slot)
        c = colour[rep]
        for w in range(planes):
            z = w + core * (planes - 1 - 2 * w)
            m = lane_even(half, columns, z + c)
            for k in range(3):
                even, odd = folded(spin, (rep, k, z), half)
                a = jnp.where(m, even, odd)
                b = jnp.where(m, odd, even)
                if w == 0:
                    sx[0, k], sx[2, k] = b, a
                elif w == 1:
                    sx[1, k], am[0, k] = b, a
                elif w == planes - 2:
                    si[1, k], am[1, k] = b, a
                else:
                    si[0, k], si[2, k] = b, a


def bond_send_kernel(planes, coup, cx, ci):
    core = core_index()
    top = planes - 1
    zx = core * top
    zi = top - zx
    for ref, z, near, outer in (
        (cx, zx, core * (top - 1), zx),
        (ci, zi, (1 - core) * (top - 1), zi),
    ):
        ref[0] = coup[0, z]
        ref[1] = coup[1, z]
        ref[2] = coup[2, near]
        ref[3] = coup[2, outer]


def weight_kernel(planes, half, coup, rcx, rci, weights):
    core = core_index()
    columns = coup.shape[-1]
    top = planes - 1
    first = core == 0

    def zbond(m):
        if m == -1:
            return folded(rcx, (2,), half)
        if m == planes + 1:
            return folded(rci, (2,), half)
        if m == 0:
            ours, theirs = folded(coup, (2, top), half), folded(rcx, (3,), half)
            return tuple(jnp.where(first, t, o) for o, t in zip(ours, theirs))
        if m == planes:
            ours, theirs = folded(coup, (2, top), half), folded(rci, (3,), half)
            return tuple(jnp.where(first, o, t) for o, t in zip(ours, theirs))
        return folded(coup, (2, (m - 1) + core * (top - 2 * m + 1)), half)

    below = zbond(-1)
    for w in range(-1, planes + 1):
        above = zbond(w + 1)
        if w == -1:
            jx, jy = folded(rcx, (0,), half), folded(rcx, (1,), half)
        elif w == planes:
            jx, jy = folded(rci, (0,), half), folded(rci, (1,), half)
        else:
            z = w + core * (top - 2 * w)
            jx, jy = folded(coup, (0, z), half), folded(coup, (1, z), half)
        up_odd = pltpu.roll(jy[1], 1, 0)
        for q in (0, 1):
            m = lane_even(half, columns, q + w + 1 + 1)
            weights[q, w + 1, 0] = jnp.where(m, jx[0], jx[1])
            weights[q, w + 1, 1] = pltpu.roll(jnp.where(m, jx[1], jx[0]), 1, 1)
            weights[q, w + 1, 2] = jy[0]
            weights[q, w + 1, 3] = jnp.where(m, up_odd, jy[1])
            weights[q, w + 1, 4] = jnp.where(m, above[0], above[1])
            weights[q, w + 1, 5] = jnp.where(m, below[0], below[1])
        below = above


def field(get, weights, q, w):
    total = []
    for k in range(3):
        o = get(w, k)
        half, columns = o.shape
        m = lane_even(half, columns, q + w + 2)
        side = jnp.where(m, pltpu.roll(o, 1, 0), pltpu.roll(o, half - 1, 0))
        h = weights[q, w + 1, 0] * pltpu.roll(o, columns - 1, 1)
        h = h + weights[q, w + 1, 1] * pltpu.roll(o, 1, 1)
        h = h + weights[q, w + 1, 2] * o
        h = h + weights[q, w + 1, 3] * side
        h = h + weights[q, w + 1, 4] * get(w + 1, k)
        h = h + weights[q, w + 1, 5] * get(w - 1, k)
        total.append(h)
    return total


def dot3(a, b):
    return a[0] * b[0] + a[1] * b[1] + a[2] * b[2]


def reflect(s, h):
    f = 2.0 * dot3(s, h) / jnp.maximum(dot3(h, h), 0.01)
    return [f * h[k] - s[k] for k in range(3)]


def first_colour(swap, colour, slot):
    return colour[slot_replica(swap, slot)] ^ core_index()


def second_planes(planes, sx, si, rx, ri):
    def get(w, k):
        if w < 0:
            return rx[-1 - w, k]
        if w < 2:
            return sx[w, k]
        if w < planes:
            return si[planes - 1 - w, k]
        return ri[w - planes, k]

    return get


def relax_kernel(planes, slot, first, *refs):
    swap, colour, weights, sx, si, rx, ri, a_old, a_new, bx, bi = refs
    q = first_colour(swap, colour, slot)
    get_b = second_planes(planes, sx, si, rx, ri)

    def get_a(w, k):
        if not first:
            return a_old[w + 1, k]
        if w == -1:
            return rx[2, k]
        if w == 0:
            return sx[2, k]
        if w == planes - 1:
            return si[2, k]
        if w == planes:
            return ri[2, k]
        return a_old[w - 1, k]

    for w in range(-1, planes + 1):
        h = field(get_b, weights, q, w)
        new = reflect([get_a(w, k) for k in range(3)], h)
        for k in range(3):
            a_new[w + 1, k] = new[k]
    for w in range(planes):
        h = field(lambda v, k: a_new[v + 1, k], weights, 1 - q, w)
        new = reflect([get_b(w, k) for k in range(3)], h)
        for k in range(3):
            if w < 2:
                bx[w, k] = new[k]
            else:
                bi[planes - 1 - w, k] = new[k]


SIN = (1.0, -1 / 6, 1 / 120, -1 / 5040, 1 / 362880, -1 / 39916800, 1 / 6227020800)
COS = (1.0, -1 / 2, 1 / 24, -1 / 720, 1 / 40320, -1 / 3628800, 1 / 479001600, -1 / 87178291200)


def series(coefficients, y):
    total = coefficients[-1]
    for value in coefficients[-2::-1]:
        total = total * y + value
    return total


def trial(height, angle):
    t = 0.5 * angle
    y = t * t
    s = t * series(SIN, y)
    c = series(COS, y)
    q = jnp.sqrt(jnp.maximum(1.0 - height * height, 0.0))
    return q * (1.0 - 2.0 * (s * s)), q * (2.0 * (s * c))


def trial_kernel(planes, half, slot, swap, colour, level, height, angle, ta, tb, dx, di):
    core = core_index()
    rep = slot_replica(swap, slot)
    c = colour[rep]
    columns = level.shape[-1]
    for w in range(planes):
        z = w + core * (planes - 1 - 2 * w)
        m = lane_even(half, columns, z + c)
        a, b = [], []
        for ref in (level, height, angle):
            even, odd = folded(ref, (rep, z), half)
            a.append(jnp.where(m, even, odd))
            b.append(jnp.where(m, odd, even))
        if w == 0 or w == planes - 1:
            for i in range(3):
                (dx if w == 0 else di)[i] = a[i]
        for t, (lev, hei, ang) in ((ta, a), (tb, b)):
            ux, uy = trial(hei, ang)
            t[w, 0], t[w, 1], t[w, 2], t[w, 3] = ux, uy, hei, lev


def heated(h, u, level, beta):
    m = jnp.maximum(dot3(h, h), 0.01)
    inverse = lax.rsqrt(m)
    e = [h[k] * inverse for k in range(3)]
    reach = beta * (m * inverse)
    c = 1.0 + jnp.log(1.0 + level * (jnp.exp(-2.0 * reach) - 1.0)) / reach
    along = dot3(u, e)
    t = [u[k] - along * e[k] for k in range(3)]
    f = jnp.sqrt(jnp.maximum(1.0 - c * c, 0.0)) * lax.rsqrt(jnp.maximum(dot3(t, t), 0.0001))
    return [c * e[k] + f * t[k] for k in range(3)]


def heat_kernel(planes, slot, *refs):
    swap, colour, betas, weights, sx, si, rx, ri, ta, tb, rdx, rdi, a_out, b_out, e_out, ah = refs
    q = first_colour(swap, colour, slot)
    beta = betas[slot_replica(swap, slot)]
    get_b = second_planes(planes, sx, si, rx, ri)

    def get_a(w, k):
        if w < 0:
            return ah[0, k]
        return ah[1, k] if w == planes else a_out[w, k]

    for w in range(-1, planes + 1):
        h = field(get_b, weights, q, w)
        if 0 <= w < planes:
            u, level = [ta[w, k] for k in range(3)], ta[w, 3]
        else:
            d = rdx if w < 0 else rdi
            ux, uy = trial(d[1], d[2])
            u, level = [ux, uy, d[1]], d[0]
        new = heated(h, u, level, beta)
        for k in range(3):
            if w < 0:
                ah[0, k] = new[k]
            elif w == planes:
                ah[1, k] = new[k]
            else:
                a_out[w, k] = new[k]
    energy = None
    for w in range(planes):
        h = field(get_a, weights, 1 - q, w)
        new = heated(h, [tb[w, k] for k in range(3)], tb[w, 3], beta)
        for k in range(3):
            b_out[w, k] = new[k]
        term = dot3(new, h)
        energy = term if energy is None else energy + term
    e_out[...] = jnp.full(e_out.shape, -jnp.sum(energy), F32)


def spread_kernel(e0, e1, out):
    lane = lax.broadcasted_iota(jnp.int32, out.shape, 1)
    out[...] = jnp.where(lane == 0, e0[:, :2], e1[:, :2])


def out_kernel(planes, half, *refs):
    swap, colour, from_below, from_above, a0, b0, a1, b1, ra0, rb0, ra1, rb1, out = refs
    core = core_index()
    columns = out.shape[-1]
    place = lax.axis_index("temp")
    take0 = (from_below[0] > 0.5) & (place != 0)
    take1 = (swap[1] != 0) & (place != lax.axis_size("temp") - 1)

    def write(slot, a, b, c):
        for w in range(planes):
            z = w + core * (planes - 1 - 2 * w)
            m = lane_even(half, columns, z + c)
            for k in range(3):
                va, vb = a[w, k], b[w, k]
                out[slot, k, z, pl.ds(0, half, stride=2), :] = jnp.where(m, va, vb)
                out[slot, k, z, pl.ds(1, half, stride=2), :] = jnp.where(m, vb, va)

    for slot, take, own, other, c_other in (
        (0, take0, (a0, b0), (ra0, rb0), from_below[1]),
        (1, take1, (a1, b1), (ra1, rb1), from_above[0]),
    ):

        @pl.when(take)
        def _():
            write(slot, *other, (c_other > 0.5).astype(jnp.int32))

        @pl.when(jnp.logical_not(take))
        def _():
            write(slot, *own, colour[slot_replica(swap, slot)])


def on_device(
    spin_state, couplings, inverse_temps, colour_order, heat_level, heat_height, heat_angle, swap_bits
):
    replicas, _, planes, rows, columns = spin_state.shape
    half = rows // 2
    assert replicas == 2 and planes == 4 and rows % 2 == 0 and columns % 2 == 0
    count = lax.axis_size("gz")
    temps = lax.axis_size("temp")
    in_chip = [(i, i ^ 1) for i in range(count)]
    cross = [(i, (i + (1 if i % 2 else -1)) % count) for i in range(count)]
    warmer = [(i, i + 1) for i in range(temps - 1)]
    colder = [(j, i) for i, j in warmer]

    def swap_in(value):
        return lax.ppermute(value, "gz", in_chip)

    def swap_cross(value):
        return lax.ppermute(value, "gz", cross)

    even = swap_bits[0] != 0
    c_low = jnp.where(even, colour_order[1], colour_order[0])
    c_high = jnp.where(even, colour_order[0], colour_order[1])
    note_up = jnp.stack([swap_bits[1], c_high]).astype(F32)
    note_down = jnp.stack([c_low, c_low]).astype(F32)
    from_below = lax.ppermute(note_up, "temp", warmer)
    from_above = lax.ppermute(note_down, "temp", colder)

    cx, ci = kernel_call(
        functools.partial(bond_send_kernel, planes),
        "bond_send",
        [vm(4, rows, columns)] * 2,
        [VM],
    )(couplings)
    rcx, rci = swap_cross(cx), swap_in(ci)

    piece = vm(3, 3, half, columns)
    sx0, sx1, si0, si1, am0, am1 = kernel_call(
        functools.partial(load_kernel, planes, half),
        "load",
        [piece, piece, piece, piece, vm(2, 3, half, columns), vm(2, 3, half, columns)],
        [SM, SM, VM],
    )(swap_bits, colour_order, spin_state)
    sx, si, a_now = [sx0, sx1], [si0, si1], [am0, am1]
    rx = [swap_cross(v) for v in sx]
    ri = [swap_in(v) for v in si]

    trials = []
    for slot in range(2):
        ta, tb, dx, di = kernel_call(
            functools.partial(trial_kernel, planes, half, slot),
            f"trial{slot}",
            [vm(planes, 4, half, columns)] * 2 + [vm(3, half, columns)] * 2,
            [SM, SM, VM, VM, VM],
        )(swap_bits, colour_order, heat_level, heat_height, heat_angle)
        trials.append((ta, tb, swap_cross(dx), swap_in(di)))

    (weights,) = kernel_call(
        functools.partial(weight_kernel, planes, half),
        "weights",
        [vm(2, planes + 2, 6, half, columns)],
        [VM, VM, VM],
    )(couplings, rcx, rci)

    for sweep in range(2):
        for slot in range(2):
            a_now[slot], sx[slot], si[slot] = kernel_call(
                functools.partial(relax_kernel, planes, slot, sweep == 0),
                f"relax{sweep}_{slot}",
                [vm(planes + 2, 3, half, columns), vm(2, 3, half, columns), vm(2, 3, half, columns)],
                [SM, SM] + [VM] * 6,
            )(swap_bits, colour_order, weights, sx[slot], si[slot], rx[slot], ri[slot], a_now[slot])
            rx[slot], ri[slot] = swap_cross(sx[slot]), swap_in(si[slot])

    own, received, energy = [], [], []
    for slot in range(2):
        ta, tb, rdx, rdi = trials[slot]
        a, b, e = pl.pallas_call(
            functools.partial(heat_kernel, planes, slot),
            name=f"heat{slot}",
            out_shape=[vm(planes, 3, half, columns)] * 2 + [vm(1, 128)],
            in_specs=[SM, SM, SM] + [VM] * 9,
            out_specs=[VM] * 3,
            scratch_shapes=[pltpu.VMEM((2, 3, half, columns), F32)],
            compiler_params=pltpu.CompilerParams(vmem_limit_bytes=24 * 1024 * 1024),
        )(
            swap_bits, colour_order, inverse_temps, weights,
            sx[slot], si[slot], rx[slot], ri[slot], ta, tb, rdx, rdi,
        )
        way = colder if slot == 0 else warmer
        own.append((a, b))
        received.append((lax.ppermute(a, "temp", way), lax.ppermute(b, "temp", way)))
        energy.append(e)

    (copies,) = kernel_call(spread_kernel, "spread", [vm(count, 2)], [VM, VM])(*energy)
    parts = lax.all_to_all(copies, "gz", split_axis=0, concat_axis=0, tiled=True)
    total_sites = float(columns * rows * planes * count)
    energy_now = jnp.sum(parts, axis=0) / total_sites
    below_energy = lax.ppermute(energy_now[1:], "temp", warmer)
    above_energy = lax.ppermute(energy_now[:1], "temp", colder)
    place = lax.axis_index("temp")
    take0 = (from_below[0] > 0.5) & (place != 0)
    take1 = (swap_bits[1] != 0) & (place != temps - 1)
    energies = jnp.concatenate(
        [
            jnp.where(take0, below_energy, energy_now[:1]),
            jnp.where(take1, above_energy, energy_now[1:]),
        ]
    )

    (a0, b0), (a1, b1) = own
    (ra1, rb1), (ra0, rb0) = received
    (spin_final,) = kernel_call(
        functools.partial(out_kernel, planes, half),
        "out",
        [jax.ShapeDtypeStruct(spin_state.shape, F32)],
        [SM, SM, SM, SM] + [VM] * 8,
    )(swap_bits, colour_order, from_below, from_above, a0, b0, a1, b1, ra0, rb0, ra1, rb1)
    return spin_final, energies


def solution(mesh):
    return jax.shard_map(
        on_device,
        mesh=mesh,
        in_specs=(
            P(("group", "temp"), None, "gz", None, None),
            P(None, ("group", "gz"), None, None),
            P(("group", "temp")),
            P(("group", "temp")),
            P(("group", "temp"), "gz", None, None),
            P(("group", "temp"), "gz", None, None),
            P(("group", "temp"), "gz", None, None),
            P(("group", "temp")),
        ),
        out_specs=(P(("group", "temp"), None, "gz", None, None), P(("group", "temp"))),
        check_vma=False,
    )
```

```python
import functools

import jax
import jax.numpy as jnp
from jax import lax
from jax.experimental import pallas as pl
from jax.experimental.pallas import tpu as pltpu
from jax.sharding import PartitionSpec as P


F32 = jnp.float32
OR_SWEEPS = 2


VM = pl.BlockSpec(memory_space=pltpu.VMEM)
SM = pl.BlockSpec(memory_space=pltpu.SMEM)
ANY = pl.BlockSpec(memory_space=pl.ANY)
HBM = pl.BlockSpec(memory_space=pltpu.HBM)
PIECES = 9


def vm(*shape, dtype=F32):
    return pltpu.VMEM(shape, dtype)


def kernel_call(body, outs, in_specs, out_specs=None, scratch=(), mib=24):
    return pl.pallas_call(
        body,
        out_shape=outs,
        in_specs=in_specs,
        out_specs=out_specs if out_specs is not None else [VM] * len(outs),
        scratch_shapes=list(scratch),
        compiler_params=pltpu.CompilerParams(vmem_limit_bytes=mib * 1024 * 1024),
    )


def in_hbm(value):
    return pltpu.with_memory_space_constraint(value, pltpu.HBM)


def core_index():
    return lax.rem(lax.axis_index("gz"), 2)


def slot_replica(swap, slot):
    bit = (swap[0] != 0).astype(jnp.int32)
    return bit if slot == 0 else 1 - bit


def lane_even(rows, columns, offset):
    lane = lax.broadcasted_iota(jnp.int32, (rows, columns), 1)
    return ((lane + offset) & 1) == 0


def tile(ref, i, half):
    return ref[pl.ds(i * half, half), :]


def put(ref, i, value):
    half = value.shape[0]
    ref[pl.ds(i * half, half), :] = value


def folded(ref, index, half):
    return tuple(ref[(*index, pl.ds(s, half, stride=2), slice(None))] for s in (0, 1))


def folded_rows(ref, base, half):
    return tuple(ref[pl.ds(base + s, half, stride=2), :] for s in (0, 1))


def parity(info, half):
    columns = info.shape[-1]
    lane = lax.broadcasted_iota(jnp.int32, (half, columns), 1)
    return (lane & 1) == jnp.broadcast_to(info[0:1, :], (half, columns))


def at_plane(even, w):
    return even if w % 2 == 0 else jnp.logical_not(even)


def load_kernel(planes, half, *refs):
    (swap_h, colour_h, beta_h, spin_h, coup_h) = refs[:5]
    (p1x, p1i, p0x, p0i, am0, am1, info0, info1, beta0, beta1) = refs[5:15]
    swap, colour, betas, spin, sems = refs[15:]
    core = core_index()
    columns = spin.shape[-1]
    rows = 2 * half
    top = planes - 1
    copies = [
        pltpu.make_async_copy(swap_h, swap, sems.at[0]),
        pltpu.make_async_copy(colour_h, colour, sems.at[1]),
        pltpu.make_async_copy(beta_h, betas, sems.at[2]),
        pltpu.make_async_copy(spin_h, spin, sems.at[3]),
    ]
    zx = core * top
    zi = top - zx
    for ref, z, near, outer, sem in (
        (p1x, zx, core * (top - 1), zx, 4),
        (p1i, zi, (1 - core) * (top - 1), zi, 8),
    ):
        for i, (d, p) in enumerate(((0, z), (1, z), (2, near), (2, outer))):
            target = ref.at[pl.ds(PIECES * half + i * rows, rows), :]
            copies.append(pltpu.make_async_copy(coup_h.at[d, p], target, sems.at[sem + i]))
    for copy in copies:
        copy.start()
    for copy in copies[:4]:
        copy.wait()
    for slot, sx, si, am, info, beta in (
        (1, p1x, p1i, am1, info1, beta1),
        (0, p0x, p0i, am0, info0, beta0),
    ):
        rep = slot_replica(swap, slot)
        c = colour[rep]
        info[0:1, :] = jnp.full((1, columns), c ^ core, jnp.int32)
        info[1:2, :] = jnp.full((1, columns), (swap[1] != 0).astype(jnp.int32), jnp.int32)
        beta[...] = jnp.full(beta.shape, betas[rep], F32)
        for w in range(planes):
            z = w + core * (top - 2 * w)
            m = lane_even(half, columns, z + c)
            for k in range(3):
                even, odd = folded(spin, (rep, k, z), half)
                a = jnp.where(m, even, odd)
                b = jnp.where(m, odd, even)
                if w == 0:
                    put(sx, k, b)
                    put(sx, 6 + k, a)
                elif w == 1:
                    put(sx, 3 + k, b)
                    put(am, k, a)
                elif w == planes - 2:
                    put(si, 3 + k, b)
                    put(am, 3 + k, a)
                else:
                    put(si, k, b)
                    put(si, 6 + k, a)
    for copy in copies[4:]:
        copy.wait()


def weight_kernel(planes, half, coup, rcx, rci, info0, info1, weights0, weights1):
    core = core_index()
    top = planes - 1
    rows = 2 * half
    first = core == 0

    def sent(ref, i):
        return folded_rows(ref, PIECES * half + i * rows, half)

    def zbond(m):
        if m == -1:
            return sent(rcx, 2)
        if m == planes + 1:
            return sent(rci, 2)
        if m == 0:
            ours, theirs = folded(coup, (2, top), half), sent(rcx, 3)
            return tuple(jnp.where(first, t, o) for o, t in zip(ours, theirs))
        if m == planes:
            ours, theirs = folded(coup, (2, top), half), sent(rci, 3)
            return tuple(jnp.where(first, o, t) for o, t in zip(ours, theirs))
        return folded(coup, (2, (m - 1) + core * (top - 2 * m + 1)), half)

    below = zbond(-1)
    for w in range(-1, planes + 1):
        above = zbond(w + 1)
        if w == -1:
            jx, jy = sent(rcx, 0), sent(rcx, 1)
        elif w == planes:
            jx, jy = sent(rci, 0), sent(rci, 1)
        else:
            z = w + core * (top - 2 * w)
            jx, jy = folded(coup, (0, z), half), folded(coup, (1, z), half)
        up_odd = pltpu.roll(jy[1], 1, 0)
        for info, weights in ((info0, weights0), (info1, weights1)):
            even = parity(info, half)
            for a in (0, 1):
                if a == 1 and (w == -1 or w == planes):
                    continue
                m = at_plane(even, w + a)
                weights[a, w + 1, 0] = jnp.where(m, jx[0], jx[1])
                weights[a, w + 1, 1] = pltpu.roll(jnp.where(m, jx[1], jx[0]), 1, 1)
                weights[a, w + 1, 2] = jy[0]
                weights[a, w + 1, 3] = jnp.where(m, up_odd, jy[1])
                weights[a, w + 1, 4] = jnp.where(m, above[0], above[1])
                weights[a, w + 1, 5] = jnp.where(m, below[0], below[1])
        below = above


def field(get, weights, a, even, w):
    total = []
    m = at_plane(even, w + a)
    for k in range(3):
        o = get(w, k)
        half, columns = o.shape
        side = jnp.where(m, pltpu.roll(o, 1, 0), pltpu.roll(o, half - 1, 0))
        h = weights[a, w + 1, 0] * pltpu.roll(o, columns - 1, 1)
        h = h + weights[a, w + 1, 1] * pltpu.roll(o, 1, 1)
        h = h + weights[a, w + 1, 2] * o
        h = h + weights[a, w + 1, 3] * side
        h = h + weights[a, w + 1, 4] * get(w + 1, k)
        h = h + weights[a, w + 1, 5] * get(w - 1, k)
        total.append(h)
    return total


def dot3(a, b):
    return a[0] * b[0] + a[1] * b[1] + a[2] * b[2]


def reflect(s, h):
    f = 2.0 * dot3(s, h) / jnp.maximum(dot3(h, h), 0.01)
    return [f * h[k] - s[k] for k in range(3)]


def second_planes(planes, half, sx, si, rx, ri):
    def get(w, k):
        if w < 0:
            return tile(rx, 3 * (-1 - w) + k, half)
        if w < 2:
            return tile(sx, 3 * w + k, half)
        if w < planes:
            return tile(si, 3 * (planes - 1 - w) + k, half)
        return tile(ri, 3 * (w - planes) + k, half)

    return get


def relax_kernel(planes, half, first, *refs):
    info, weights, sx, si, rx, ri, a_old = refs[:7]
    a_new, bx, bi = refs[7:] if first else (refs[9], refs[7], refs[8])
    even = parity(info, half)
    get_b = second_planes(planes, half, sx, si, rx, ri)

    def get_a(w, k):
        if not first:
            return a_old[w + 1, k]
        if w == -1:
            return tile(rx, 6 + k, half)
        if w == 0:
            return tile(sx, 6 + k, half)
        if w == planes - 1:
            return tile(si, 6 + k, half)
        if w == planes:
            return tile(ri, 6 + k, half)
        return tile(a_old, 3 * (w - 1) + k, half)

    for w in range(-1, planes + 1):
        h = field(get_b, weights, 0, even, w)
        new = reflect([get_a(w, k) for k in range(3)], h)
        for k in range(3):
            a_new[w + 1, k] = new[k]
    for w in range(planes):
        h = field(lambda v, k: a_new[v + 1, k], weights, 1, even, w)
        new = reflect([get_b(w, k) for k in range(3)], h)
        for k in range(3):
            if w < 2:
                put(bx, 3 * w + k, new[k])
            else:
                put(bi, 3 * (planes - 1 - w) + k, new[k])


SIN = (1.0, -1 / 6, 1 / 120, -1 / 5040, 1 / 362880, -1 / 39916800, 1 / 6227020800)
COS = (1.0, -1 / 2, 1 / 24, -1 / 720, 1 / 40320, -1 / 3628800, 1 / 479001600, -1 / 87178291200)


def series(coefficients, y):
    total = coefficients[-1]
    for value in coefficients[-2::-1]:
        total = total * y + value
    return total


def trial(height, angle):
    t = 0.5 * angle
    y = t * t
    s = t * series(SIN, y)
    c = series(COS, y)
    q = jnp.sqrt(jnp.maximum(1.0 - height * height, 0.0))
    return q * (1.0 - 2.0 * (s * s)), q * (2.0 * (s * c))


def trial_kernel(planes, half, swap, colour, level, height, angle, ta0, tb0, ta1, tb1, dx, di):
    core = core_index()
    columns = level.shape[-1]
    for slot, ta, tb in ((0, ta0, tb0), (1, ta1, tb1)):
        rep = slot_replica(swap, slot)
        c = colour[rep]
        for w in range(planes):
            z = w + core * (planes - 1 - 2 * w)
            m = lane_even(half, columns, z + c)
            a, b = [], []
            for ref in (level, height, angle):
                even, odd = folded(ref, (rep, z), half)
                a.append(jnp.where(m, even, odd))
                b.append(jnp.where(m, odd, even))
            if w == 0 or w == planes - 1:
                for i in range(3):
                    put(dx if w == 0 else di, 3 * slot + i, a[i])
            for t, (lev, hei, ang) in ((ta, a), (tb, b)):
                ux, uy = trial(hei, ang)
                t[w, 0], t[w, 1], t[w, 2], t[w, 3] = ux, uy, hei, lev


def heated(h, u, level, beta):
    m = jnp.maximum(dot3(h, h), 0.01)
    inverse = lax.rsqrt(m)
    e = [h[k] * inverse for k in range(3)]
    reach = beta * (m * inverse)
    c = 1.0 + jnp.log(1.0 + level * (jnp.exp(-2.0 * reach) - 1.0)) / reach
    along = dot3(u, e)
    t = [u[k] - along * e[k] for k in range(3)]
    f = jnp.sqrt(jnp.maximum(1.0 - c * c, 0.0)) * lax.rsqrt(jnp.maximum(dot3(t, t), 0.0001))
    return [c * e[k] + f * t[k] for k in range(3)]


def inner_kernel(planes, half, info, betas, weights, sx, si, ta, out):
    even = parity(info, half)
    columns = info.shape[-1]
    beta = jnp.broadcast_to(betas[0:1, :], (half, columns))
    get_b = second_planes(planes, half, sx, si, None, None)
    for w in range(1, planes - 1):
        h = field(get_b, weights, 0, even, w)
        new = heated(h, [ta[w, k] for k in range(3)], ta[w, 3], beta)
        for k in range(3):
            put(out, 3 * (w - 1) + k, new[k])
    out[pl.ds(3 * (planes - 2) * half, 8), :] = info[...].astype(F32)


def heat_kernel(planes, half, slot, *refs):
    info, betas, weights, sx, si, rx, ri, ta, tb, rdx, rdi, inner, out, e_out, ah = refs
    even = parity(info, half)
    columns = info.shape[-1]
    beta = jnp.broadcast_to(betas[0:1, :], (half, columns))
    get_b = second_planes(planes, half, sx, si, rx, ri)

    def get_a(w, k):
        if w < 0:
            return ah[0, k]
        if w == planes:
            return ah[1, k]
        if w == 0:
            return tile(out, k, half)
        if w == planes - 1:
            return tile(out, 3 + k, half)
        return tile(inner, 3 * (w - 1) + k, half)

    for w in (-1, 0, planes - 1, planes):
        h = field(get_b, weights, 0, even, w)
        if 0 <= w < planes:
            u, level = [ta[w, k] for k in range(3)], ta[w, 3]
        else:
            d = rdx if w < 0 else rdi
            height = tile(d, 3 * slot + 1, half)
            ux, uy = trial(height, tile(d, 3 * slot + 2, half))
            u, level = [ux, uy, height], tile(d, 3 * slot, half)
        new = heated(h, u, level, beta)
        for k in range(3):
            if w < 0:
                ah[0, k] = new[k]
            elif w == planes:
                ah[1, k] = new[k]
            else:
                put(out, (0 if w == 0 else 3) + k, new[k])
    energy = None
    for w in range(planes):
        h = field(get_a, weights, 1, even, w)
        new = heated(h, [tb[w, k] for k in range(3)], tb[w, 3], beta)
        for k in range(3):
            put(out, 6 + 3 * w + k, new[k])
        term = dot3(new, h)
        energy = term if energy is None else energy + term
    e_out[...] = jnp.full(e_out.shape, -jnp.sum(energy), F32)


def decide_kernel(notes, e0, e1, re0, re1, ri0, ri1, info0, info1, copies, sel):
    place = lax.axis_index("temp")
    lower = place != 0
    upper = place != lax.axis_size("temp") - 1
    n0, n1 = ri0[pl.ds(notes, 8), :], ri1[pl.ds(notes, 8), :]
    take0 = jnp.logical_and(n0[1:2, :] > 0.5, lower)
    take1 = jnp.logical_and(info0[1:2, :] > 0, upper)
    f0 = jnp.where(take0, re0[0:1, :], e0[0:1, :])
    f1 = jnp.where(take1, re1[0:1, :], e1[0:1, :])
    lane = lax.broadcasted_iota(jnp.int32, copies.shape, 1)
    shape = copies.shape
    copies[...] = jnp.where(
        lane == 0,
        jnp.broadcast_to(f0[:, : shape[1]], shape),
        jnp.broadcast_to(f1[:, : shape[1]], shape),
    )
    c0 = jnp.where(take0, n0[0:1, :], info0[0:1, :].astype(F32))
    c1 = jnp.where(take1, n1[0:1, :], info1[0:1, :].astype(F32))
    for i, v in enumerate((take0.astype(F32), take1.astype(F32), c0, c1)):
        sel[i] = (jnp.max(v) > 0.5).astype(jnp.int32)


def out_kernel(planes, half, *refs):
    sel, i0, i1, o0, o1, ri0, ri1, ro0, ro1, out_h, inner, outer, out, sems = refs
    core = core_index()
    columns = out.shape[-1]
    sources = (((i0, o0), (ri0, ro0)), ((i1, o1), (ri1, ro1)))

    def pull(slot, other):
        return [
            pltpu.make_async_copy(sources[slot][other][0], inner.at[slot], sems.at[slot]),
            pltpu.make_async_copy(sources[slot][other][1], outer.at[slot], sems.at[2 + slot]),
        ]

    for slot in range(2):
        for other in range(2):

            @pl.when(sel[slot] == other)
            def _():
                for copy in pull(slot, other):
                    copy.start()

    pushes = []
    for slot in range(2):
        for copy in pull(slot, 0):
            copy.wait()
        c = sel[2 + slot]
        a_of, b_of = inner.at[slot], outer.at[slot]
        for w in range(planes):
            z = w + core * (planes - 1 - 2 * w)
            m = lane_even(half, columns, w + c)
            for k in range(3):
                if 0 < w < planes - 1:
                    a = tile(a_of, 3 * (w - 1) + k, half)
                else:
                    a = tile(b_of, (0 if w == 0 else 3) + k, half)
                b = tile(b_of, 6 + 3 * w + k, half)
                out[slot, k, z, pl.ds(0, half, stride=2), :] = jnp.where(m, a, b)
                out[slot, k, z, pl.ds(1, half, stride=2), :] = jnp.where(m, b, a)
        push = pltpu.make_async_copy(out.at[slot], out_h.at[slot], sems.at[4 + slot])
        push.start()
        pushes.append(push)
    for push in pushes:
        push.wait()


def step(
    spin_state, couplings, inverse_temps, colour_order, heat_level, heat_height, heat_angle, swap_bits
):
    replicas, _, planes, rows, columns = spin_state.shape
    half = rows // 2
    assert replicas == 2 and planes == 4 and rows % 2 == 0 and columns % 2 == 0
    count = lax.axis_size("gz")
    temps = lax.axis_size("temp")
    in_chip = [(i, i ^ 1) for i in range(count)]
    cross = [(i, (i + (1 if i % 2 else -1)) % count) for i in range(count)]
    warmer = [(i, i + 1) for i in range(temps - 1)]
    colder = [(j, i) for i, j in warmer]

    def swap_in(value):
        return lax.ppermute(value, "gz", in_chip)

    def swap_cross(value):
        return lax.ppermute(value, "gz", cross)

    def away(value, slot):
        return lax.ppermute(value, "temp", warmer if slot else colder)

    spins = PIECES * half
    both = spins + 4 * rows
    p1x, p1i, p0x, p0i, am0, am1, info0, info1, beta0, beta1 = kernel_call(
        functools.partial(load_kernel, planes, half),
        [vm(both, columns)] * 2
        + [vm(spins, columns)] * 2
        + [vm(6 * half, columns)] * 2
        + [vm(8, columns, dtype=jnp.int32)] * 2
        + [vm(8, columns)] * 2,
        [HBM] * 5,
        scratch=[
            pltpu.SMEM((replicas,), jnp.int32),
            pltpu.SMEM((replicas,), jnp.int32),
            pltpu.SMEM((replicas,), F32),
            pltpu.VMEM(spin_state.shape, F32),
            pltpu.SemaphoreType.DMA((12,)),
        ],
    )(*(in_hbm(v) for v in (swap_bits, colour_order, inverse_temps, spin_state, couplings)))
    info, beta = [info0, info1], [beta0, beta1]
    sx, si, a_now = [p0x, p1x], [p0i, p1i], [am0, am1]
    rx1, ri1 = swap_cross(p1x), swap_in(p1i)
    rx0, ri0 = swap_cross(p0x), swap_in(p0i)
    rx, ri = [rx0, rx1], [ri0, ri1]

    ta0, tb0, ta1, tb1, dx, di = kernel_call(
        functools.partial(trial_kernel, planes, half),
        [vm(planes, 4, half, columns)] * 4 + [vm(6 * half, columns)] * 2,
        [SM, SM, VM, VM, VM],
    )(swap_bits, colour_order, heat_level, heat_height, heat_angle)
    trial_a, trial_b = [ta0, ta1], [tb0, tb1]
    rdx, rdi = swap_cross(dx), swap_in(di)

    weights = kernel_call(
        functools.partial(weight_kernel, planes, half),
        [vm(2, planes + 2, 6, half, columns)] * 2,
        [VM] * 5,
    )(couplings, rx1, ri1, info0, info1)

    for sweep in range(OR_SWEEPS):
        for slot in (1, 0):
            first = sweep == 0
            updated = vm(planes + 2, 3, half, columns)
            *a_next, sx[slot], si[slot] = kernel_call(
                functools.partial(relax_kernel, planes, half, first),
                [updated] * first + [vm(6 * half, columns)] * 2,
                [VM] * 7,
                scratch=[updated] * (not first),
            )(info[slot], weights[slot], sx[slot], si[slot], rx[slot], ri[slot], a_now[slot])
            a_now[slot] = a_next[0] if first else None
            rx[slot], ri[slot] = swap_cross(sx[slot]), swap_in(si[slot])

    inner, r_inner = [None] * 2, [None] * 2
    for slot in (1, 0):
        (inner[slot],) = kernel_call(
            functools.partial(inner_kernel, planes, half),
            [jax.ShapeDtypeStruct((3 * (planes - 2) * half + 8, columns), F32)],
            [VM] * 6,
        )(info[slot], beta[slot], weights[slot], sx[slot], si[slot], trial_a[slot])
        r_inner[slot] = away(inner[slot], slot)
    outer, r_outer, energy, r_energy = [None] * 2, [None] * 2, [None] * 2, [None] * 2
    for slot in (1, 0):
        outer[slot], energy[slot] = kernel_call(
            functools.partial(heat_kernel, planes, half, slot),
            [jax.ShapeDtypeStruct((18 * half, columns), F32), vm(8, columns)],
            [VM] * 12,
            scratch=[pltpu.VMEM((2, 3, half, columns), F32)],
        )(
            info[slot], beta[slot], weights[slot], sx[slot], si[slot], rx[slot], ri[slot],
            trial_a[slot], trial_b[slot], rdx, rdi, inner[slot],
        )
        r_energy[slot] = away(energy[slot], slot)
        r_outer[slot] = away(outer[slot], slot)
    r_inner, r_outer, r_energy = r_inner[::-1], r_outer[::-1], r_energy[::-1]

    copies, sel = kernel_call(
        functools.partial(decide_kernel, 3 * (planes - 2) * half),
        [vm(count, 2), jax.ShapeDtypeStruct((4,), jnp.int32)],
        [VM] * 8,
        out_specs=[VM, SM],
    )(energy[0], energy[1], r_energy[0], r_energy[1], r_inner[0], r_inner[1], info0, info1)
    parts = lax.all_to_all(copies, "gz", split_axis=0, concat_axis=0, tiled=True)
    energies = jnp.sum(parts, axis=0) / float(columns * rows * planes * count)

    (spin_final,) = kernel_call(
        functools.partial(out_kernel, planes, half),
        [jax.ShapeDtypeStruct(spin_state.shape, F32)],
        [SM] + [ANY] * 8,
        out_specs=[ANY],
        scratch=[
            pltpu.VMEM((2, *inner[0].shape), F32),
            pltpu.VMEM((2, *outer[0].shape), F32),
            pltpu.VMEM(spin_state.shape, F32),
            pltpu.SemaphoreType.DMA((6,)),
        ],
    )(sel, inner[0], inner[1], outer[0], outer[1], r_inner[0], r_inner[1], r_outer[0], r_outer[1])
    return spin_final, energies


def solution(mesh):
    return jax.shard_map(
        step,
        mesh=mesh,
        in_specs=(
            P(("group", "temp"), None, "gz", None, None),
            P(None, ("group", "gz"), None, None),
            P(("group", "temp")),
            P(("group", "temp")),
            P(("group", "temp"), "gz", None, None),
            P(("group", "temp"), "gz", None, None),
            P(("group", "temp"), "gz", None, None),
            P(("group", "temp")),
        ),
        out_specs=(P(("group", "temp"), None, "gz", None, None), P(("group", "temp"))),
        check_vma=False,
    )
```

```python
import functools

import jax
import jax.numpy as jnp
from jax import lax
from jax.experimental import pallas as pl
from jax.experimental.pallas import tpu as pltpu
from jax.sharding import PartitionSpec as P


F32 = jnp.float32
OR_SWEEPS = 2


VM = pl.BlockSpec(memory_space=pltpu.VMEM)
SM = pl.BlockSpec(memory_space=pltpu.SMEM)
ANY = pl.BlockSpec(memory_space=pl.ANY)
HBM = pl.BlockSpec(memory_space=pltpu.HBM)
PIECES = 9
EARLY = 15
LATE = 9


def vm(*shape, dtype=F32):
    return pltpu.VMEM(shape, dtype)


def kernel_call(body, outs, in_specs, out_specs=None, scratch=(), mib=24):
    return pl.pallas_call(
        body,
        out_shape=outs,
        in_specs=in_specs,
        out_specs=out_specs if out_specs is not None else [VM] * len(outs),
        scratch_shapes=list(scratch),
        compiler_params=pltpu.CompilerParams(vmem_limit_bytes=mib * 1024 * 1024),
    )


def in_hbm(value):
    return pltpu.with_memory_space_constraint(value, pltpu.HBM)


def core_index():
    return lax.rem(lax.axis_index("gz"), 2)


def slot_of(u):
    odd = lax.rem(lax.axis_index("temp"), 2)
    return 1 - odd if u == 0 else odd


def slot_replica(swap, u):
    return slot_of(u) ^ (swap[0] != 0).astype(jnp.int32)


def lane_even(rows, columns, offset):
    lane = lax.broadcasted_iota(jnp.int32, (rows, columns), 1)
    return ((lane + offset) & 1) == 0


def tile(ref, i, half):
    return ref[pl.ds(i * half, half), :]


def put(ref, i, value):
    half = value.shape[0]
    ref[pl.ds(i * half, half), :] = value


def folded(ref, index, half):
    return tuple(ref[(*index, pl.ds(s, half, stride=2), slice(None))] for s in (0, 1))


def folded_rows(ref, base, half):
    return tuple(ref[pl.ds(base + s, half, stride=2), :] for s in (0, 1))


def parity(info, half):
    columns = info.shape[-1]
    lane = lax.broadcasted_iota(jnp.int32, (half, columns), 1)
    return (lane & 1) == jnp.broadcast_to(info[0:1, :], (half, columns))


def at_plane(even, w):
    return even if w % 2 == 0 else jnp.logical_not(even)


def load_kernel(planes, half, *refs):
    (swap_h, colour_h, beta_h, spin_h, coup_h) = refs[:5]
    (p0x, p0i, p1x, p1i, am0, am1, info0, info1, beta0, beta1) = refs[5:15]
    swap, colour, betas, spin, sems = refs[15:]
    core = core_index()
    columns = spin.shape[-1]
    rows = 2 * half
    top = planes - 1
    scalars = [
        pltpu.make_async_copy(swap_h, swap, sems.at[0]),
        pltpu.make_async_copy(colour_h, colour, sems.at[1]),
        pltpu.make_async_copy(beta_h, betas, sems.at[2]),
    ]
    spins = [
        pltpu.make_async_copy(spin_h.at[:, :, w + core * (top - 2 * w)], spin.at[w], sems.at[3 + w])
        for w in range(planes)
    ]
    bonds = []
    zx = core * top
    zi = top - zx
    for ref, z, near, outer, sem in (
        (p0x, zx, core * (top - 1), zx, 3 + planes),
        (p0i, zi, (1 - core) * (top - 1), zi, 7 + planes),
    ):
        for i, (d, p) in enumerate(((0, z), (1, z), (2, near), (2, outer))):
            target = ref.at[pl.ds(PIECES * half + i * rows, rows), :]
            bonds.append(pltpu.make_async_copy(coup_h.at[d, p], target, sems.at[sem + i]))
    for copy in scalars + spins + bonds:
        copy.start()
    for copy in scalars:
        copy.wait()
    reps, masks = [], []
    for u, info, beta in ((0, info0, beta0), (1, info1, beta1)):
        rep = slot_replica(swap, u)
        c = colour[rep] ^ core
        info[0:1, :] = jnp.full((1, columns), c, jnp.int32)
        info[1:2, :] = jnp.full((1, columns), (swap[1] != 0).astype(jnp.int32), jnp.int32)
        beta[...] = jnp.full(beta.shape, betas[rep], F32)
        reps.append(rep)
        masks.append(lane_even(half, columns, c))
    for w in range(planes):
        spins[w].wait()
        for u, sx, si, am in ((0, p0x, p0i, am0), (1, p1x, p1i, am1)):
            m = at_plane(masks[u], w)
            for k in range(3):
                even, odd = folded(spin, (w, reps[u], k), half)
                a = jnp.where(m, even, odd)
                b = jnp.where(m, odd, even)
                if w == 0:
                    put(sx, k, b)
                    put(sx, 6 + k, a)
                elif w == 1:
                    put(sx, 3 + k, b)
                    put(am, k, a)
                elif w == planes - 2:
                    put(si, 3 + k, b)
                    put(am, 3 + k, a)
                else:
                    put(si, k, b)
                    put(si, 6 + k, a)
    for copy in bonds:
        copy.wait()


def weight_kernel(planes, half, in_chip, *refs):
    coup, sent_ref, info0, info1, weights0, weights1 = refs
    core = core_index()
    top = planes - 1
    rows = 2 * half
    first = core == 0

    def sent(i):
        return folded_rows(sent_ref, PIECES * half + i * rows, half)

    def zbond(m):
        if m in (-1, planes + 1):
            return sent(2)
        if m in (0, planes):
            ours, theirs = folded(coup, (2, top), half), sent(3)
            mine = first if m == planes else jnp.logical_not(first)
            return tuple(jnp.where(mine, o, t) for o, t in zip(ours, theirs))
        return folded(coup, (2, (m - 1) + core * (top - 2 * m + 1)), half)

    span = range(1, planes + 1) if in_chip else range(-1, 1)
    below = zbond(span[0])
    for i, w in enumerate(span):
        above = zbond(w + 1)
        if w in (-1, planes):
            jx, jy = sent(0), sent(1)
        else:
            z = w + core * (top - 2 * w)
            jx, jy = folded(coup, (0, z), half), folded(coup, (1, z), half)
        up_odd = pltpu.roll(jy[1], 1, 0)
        for info, weights in ((info0, weights0), (info1, weights1)):
            even = parity(info, half)
            for a in (0, 1):
                if a == 1 and w in (-1, planes):
                    continue
                m = at_plane(even, w + a)
                weights[a, i, 0] = jnp.where(m, jx[0], jx[1])
                weights[a, i, 1] = pltpu.roll(jnp.where(m, jx[1], jx[0]), 1, 1)
                weights[a, i, 2] = jy[0]
                weights[a, i, 3] = jnp.where(m, up_odd, jy[1])
                weights[a, i, 4] = jnp.where(m, above[0], above[1])
                weights[a, i, 5] = jnp.where(m, below[0], below[1])
        below = above


def field(get, weight, a, even, w):
    total = []
    m = at_plane(even, w + a)
    for k in range(3):
        o = get(w, k)
        half, columns = o.shape
        side = jnp.where(m, pltpu.roll(o, 1, 0), pltpu.roll(o, half - 1, 0))
        h = weight(a, w, 0) * pltpu.roll(o, columns - 1, 1)
        h = h + weight(a, w, 1) * pltpu.roll(o, 1, 1)
        h = h + weight(a, w, 2) * o
        h = h + weight(a, w, 3) * side
        h = h + weight(a, w, 4) * get(w + 1, k)
        h = h + weight(a, w, 5) * get(w - 1, k)
        total.append(h)
    return total


def weight_of(w_in, w_x):
    return lambda a, w, i: w_in[a, w - 1, i] if w > 0 else w_x[a, w + 1, i]


def dot3(a, b):
    return a[0] * b[0] + a[1] * b[1] + a[2] * b[2]


def reflect(s, h):
    f = 2.0 * dot3(s, h) / jnp.maximum(dot3(h, h), 0.01)
    return [f * h[k] - s[k] for k in range(3)]


def second_planes(planes, half, sx, si, rx, ri):
    def get(w, k):
        if w < 0:
            return tile(rx, 3 * (-1 - w) + k, half)
        if w < 2:
            return tile(sx, 3 * w + k, half)
        if w < planes:
            return tile(si, 3 * (planes - 1 - w) + k, half)
        return tile(ri, 3 * (w - planes) + k, half)

    return get


def relax_early(planes, half, first, *refs):
    info, w_in, sx, si, ri, a_old, a_new, bi = refs
    even = parity(info, half)
    weight = weight_of(w_in, None)
    get_b = second_planes(planes, half, sx, si, None, ri)

    def get_a(w, k):
        if not first:
            return tile(a_old, 3 * (w - 1) + k, half)
        if w == planes - 1:
            return tile(si, 6 + k, half)
        if w == planes:
            return tile(ri, 6 + k, half)
        return tile(a_old, 3 * (w - 1) + k, half)

    for w in range(1, planes + 1):
        h = field(get_b, weight, 0, even, w)
        new = reflect([get_a(w, k) for k in range(3)], h)
        for k in range(3):
            put(a_new, 3 * (w - 1) + k, new[k])
    for w in range(2, planes):
        h = field(lambda v, k: tile(a_new, 3 * (v - 1) + k, half), weight, 1, even, w)
        new = reflect([get_b(w, k) for k in range(3)], h)
        for k in range(3):
            put(bi, 3 * (planes - 1 - w) + k, new[k])


def relax_late(planes, half, first, *refs):
    info, w_in, w_x, sx, rx, a_in = refs[:6]
    a_old, a_new, bx = (None, *refs[6:]) if first else (refs[6], refs[8], refs[7])
    even = parity(info, half)
    weight = weight_of(w_in, w_x)
    get_b = second_planes(planes, half, sx, None, rx, None)

    def get_a(w, k):
        if not first:
            return tile(a_old, 3 * (w + 1) + k, half)
        return tile(rx if w < 0 else sx, 6 + k, half)

    for w in (-1, 0):
        h = field(get_b, weight, 0, even, w)
        new = reflect([get_a(w, k) for k in range(3)], h)
        for k in range(3):
            put(a_new, 3 * (w + 1) + k, new[k])

    def get_new(w, k):
        return tile(a_new, 3 * (w + 1) + k, half) if w < 1 else tile(a_in, 3 * (w - 1) + k, half)

    for w in (0, 1):
        h = field(get_new, weight, 1, even, w)
        new = reflect([get_b(w, k) for k in range(3)], h)
        for k in range(3):
            put(bx, 3 * w + k, new[k])


SIN = (1.0, -1 / 6, 1 / 120, -1 / 5040, 1 / 362880, -1 / 39916800, 1 / 6227020800)
COS = (1.0, -1 / 2, 1 / 24, -1 / 720, 1 / 40320, -1 / 3628800, 1 / 479001600, -1 / 87178291200)


def series(coefficients, y):
    total = coefficients[-1]
    for value in coefficients[-2::-1]:
        total = total * y + value
    return total


def trial(height, angle):
    t = 0.5 * angle
    y = t * t
    s = t * series(SIN, y)
    c = series(COS, y)
    q = jnp.sqrt(jnp.maximum(1.0 - height * height, 0.0))
    return q * (1.0 - 2.0 * (s * s)), q * (2.0 * (s * c))


def trial_kernel(planes, half, swap, colour, level, height, angle, ta0, tb0, ta1, tb1, dx, di):
    core = core_index()
    columns = level.shape[-1]
    for u, ta, tb in ((0, ta0, tb0), (1, ta1, tb1)):
        rep = slot_replica(swap, u)
        c = colour[rep]
        for w in range(planes):
            z = w + core * (planes - 1 - 2 * w)
            m = lane_even(half, columns, z + c)
            a, b = [], []
            for ref in (level, height, angle):
                even, odd = folded(ref, (rep, z), half)
                a.append(jnp.where(m, even, odd))
                b.append(jnp.where(m, odd, even))
            if w == 0 or w == planes - 1:
                for i in range(3):
                    put(dx if w == 0 else di, 3 * u + i, a[i])
            for t, (lev, hei, ang) in ((ta, a), (tb, b)):
                ux, uy = trial(hei, ang)
                t[w, 0], t[w, 1], t[w, 2], t[w, 3] = ux, uy, hei, lev


def trial_of(t, w):
    return [t[w, k] for k in range(3)], t[w, 3]


def trial_sent(draws, u, half):
    level, height, angle = (tile(draws, 3 * u + i, half) for i in range(3))
    ux, uy = trial(height, angle)
    return [ux, uy, height], level


def heated(h, u, level, beta):
    m = jnp.maximum(dot3(h, h), 0.01)
    inverse = lax.rsqrt(m)
    e = [h[k] * inverse for k in range(3)]
    reach = beta * (m * inverse)
    c = 1.0 + jnp.log(1.0 + level * (jnp.exp(-2.0 * reach) - 1.0)) / reach
    along = dot3(u, e)
    t = [u[k] - along * e[k] for k in range(3)]
    f = jnp.sqrt(jnp.maximum(1.0 - c * c, 0.0)) * lax.rsqrt(jnp.maximum(dot3(t, t), 0.0001))
    return [c * e[k] + f * t[k] for k in range(3)]


def heat_early(planes, half, u, *refs):
    info, betas, w_in, sx, si, ri, ta, tb, rdi, out, e_part, halo = refs
    even = parity(info, half)
    columns = info.shape[-1]
    beta = jnp.broadcast_to(betas[0:1, :], (half, columns))
    weight = weight_of(w_in, None)
    get_b = second_planes(planes, half, sx, si, None, ri)

    def get_a(w, k):
        return halo[k] if w == planes else tile(out, 3 * (w - 1) + k, half)

    for w in range(1, planes + 1):
        h = field(get_b, weight, 0, even, w)
        draw = trial_of(ta, w) if w < planes else trial_sent(rdi, u, half)
        new = heated(h, *draw, beta)
        for k in range(3):
            if w == planes:
                halo[k] = new[k]
            else:
                put(out, 3 * (w - 1) + k, new[k])
    energy = None
    for w in range(2, planes):
        h = field(get_a, weight, 1, even, w)
        new = heated(h, *trial_of(tb, w), beta)
        for k in range(3):
            put(out, 9 + 3 * (w - 2) + k, new[k])
        term = dot3(new, h)
        energy = term if energy is None else energy + term
    e_part[...] = energy
    out[pl.ds(EARLY * half, 8), :] = info[...].astype(F32)


def heat_late(planes, half, u, *refs):
    info, betas, w_in, w_x, sx, rx, ta, tb, rdx, inner, e_part = refs[:11]
    if u == 0:
        out, e_out, halo = refs[11:]
    else:
        e_other, out, e_out, halo = refs[11:]
    even = parity(info, half)
    columns = info.shape[-1]
    beta = jnp.broadcast_to(betas[0:1, :], (half, columns))
    weight = weight_of(w_in, w_x)
    get_b = second_planes(planes, half, sx, None, rx, None)

    def get_a(w, k):
        if w < 0:
            return halo[k]
        return tile(out, k, half) if w == 0 else tile(inner, 3 * (w - 1) + k, half)

    for w in (-1, 0):
        h = field(get_b, weight, 0, even, w)
        draw = trial_of(ta, w) if w >= 0 else trial_sent(rdx, u, half)
        new = heated(h, *draw, beta)
        for k in range(3):
            if w < 0:
                halo[k] = new[k]
            else:
                put(out, k, new[k])
    energy = e_part[...]
    for w in (0, 1):
        h = field(get_a, weight, 1, even, w)
        new = heated(h, *trial_of(tb, w), beta)
        for k in range(3):
            put(out, 3 + 3 * w + k, new[k])
        energy = energy + dot3(new, h)
    mine = jnp.full(e_out.shape, -jnp.sum(energy), F32)
    if u == 1:
        lane = lax.broadcasted_iota(jnp.int32, e_out.shape, 1)
        other = jnp.broadcast_to(e_other[0:1, : e_out.shape[1]], e_out.shape)
        mine = jnp.where(lane == 0, other, mine)
    e_out[...] = mine


def total_kernel(sites, parts, total):
    total[...] = jnp.sum(parts[...], axis=0, keepdims=True) / sites


def exchanged(u, info, note):
    place = lax.axis_index("temp")
    upper = slot_of(u) == 1
    ours = jnp.max(info[1:2, :]) > 0
    theirs = jnp.max(note[1:2, :]) > 0.5
    inside = jnp.where(upper, place != lax.axis_size("temp") - 1, place != 0)
    return jnp.logical_and(jnp.where(upper, ours, theirs), inside)


def out_kernel(planes, half, *refs):
    info0, info1, i0, i1, o0, o1, ri0, ri1, ro0, ro1, out_h, out, sems = refs
    core = core_index()
    columns = out.shape[-1]
    pushes = []
    for u, info, own, other in ((0, info0, (i0, o0), (ri0, ro0)), (1, info1, (i1, o1), (ri1, ro1))):
        note = ri0[pl.ds(EARLY * half, 8), :] if u == 0 else ri1[pl.ds(EARLY * half, 8), :]
        take = exchanged(u, info, note)

        def write(early, late, parities):
            even = (lax.broadcasted_iota(jnp.int32, (half, columns), 1) & 1) == jnp.broadcast_to(
                parities, (half, columns)
            )
            for w in range(planes):
                z = w + core * (planes - 1 - 2 * w)
                m = at_plane(even, w)
                for k in range(3):
                    a = tile(late, k, half) if w == 0 else tile(early, 3 * (w - 1) + k, half)
                    b = tile(late, 3 + 3 * w + k, half) if w < 2 else tile(early, 3 + 3 * w + k, half)
                    out[u, k, z, pl.ds(0, half, stride=2), :] = jnp.where(m, a, b)
                    out[u, k, z, pl.ds(1, half, stride=2), :] = jnp.where(m, b, a)

        @pl.when(take)
        def _():
            write(*other, note[0:1, :].astype(jnp.int32))

        @pl.when(jnp.logical_not(take))
        def _():
            write(*own, info[0:1, :])

        push = pltpu.make_async_copy(out.at[u], out_h.at[slot_of(u)], sems.at[u])
        push.start()
        pushes.append(push)
    for push in pushes:
        push.wait()


def energy_kernel(half, info0, info1, total, r0, r1, ri0, ri1, energies):
    final = []
    for u, info, r, ri in ((0, info0, r0, ri0), (1, info1, r1, ri1)):
        take = exchanged(u, info, ri[pl.ds(EARLY * half, 8), :])
        final.append(jnp.where(take, r[...], total[...]))
    lane = lax.broadcasted_iota(jnp.int32, energies.shape, 1)
    sums = [jnp.sum(jnp.where(lane == u, final[u], 0.0)) for u in range(2)]
    energies[...] = jnp.where(lane == slot_of(0), sums[0], sums[1])


def step(
    spin_state, couplings, inverse_temps, colour_order, heat_level, heat_height, heat_angle, swap_bits
):
    replicas, _, planes, rows, columns = spin_state.shape
    half = rows // 2
    count = lax.axis_size("gz")
    temps = lax.axis_size("temp")
    assert replicas == 2 and planes == 4 and rows % 2 == 0 and columns % 2 == 0
    assert count % 2 == 0 and temps % 2 == 0
    in_chip = [(i, i ^ 1) for i in range(count)]
    cross = [(i, (i + (1 if i % 2 else -1)) % count) for i in range(count)]
    partners = (
        [(i, i ^ 1) for i in range(temps)],
        [(i, (i + (1 if i % 2 else -1)) % temps) for i in range(temps)],
    )

    def swap_in(value):
        return lax.ppermute(value, "gz", in_chip)

    def swap_cross(value):
        return lax.ppermute(value, "gz", cross)

    def away(value, u):
        return lax.ppermute(value, "temp", partners[u])

    spins = PIECES * half
    both = spins + 4 * rows
    pair = vm(6 * half, columns)
    p0x, p0i, p1x, p1i, am0, am1, info0, info1, beta0, beta1 = kernel_call(
        functools.partial(load_kernel, planes, half),
        [vm(both, columns)] * 2
        + [vm(spins, columns)] * 2
        + [pair] * 2
        + [vm(8, columns, dtype=jnp.int32)] * 2
        + [vm(8, columns)] * 2,
        [HBM] * 5,
        scratch=[
            pltpu.SMEM((replicas,), jnp.int32),
            pltpu.SMEM((replicas,), jnp.int32),
            pltpu.SMEM((replicas,), F32),
            vm(planes, replicas, 3, rows, columns),
            pltpu.SemaphoreType.DMA((11 + planes,)),
        ],
    )(*(in_hbm(v) for v in (swap_bits, colour_order, inverse_temps, spin_state, couplings)))
    info, beta = [info0, info1], [beta0, beta1]
    sx, si, a_in, a_x = [p0x, p1x], [p0i, p1i], [am0, am1], [[], []]
    rx = [swap_cross(sx[u]) for u in range(2)]
    ri = [swap_in(si[u]) for u in range(2)]

    ta0, tb0, ta1, tb1, dx, di = kernel_call(
        functools.partial(trial_kernel, planes, half),
        [vm(planes, 4, half, columns)] * 4 + [pair] * 2,
        [SM, SM, VM, VM, VM],
    )(swap_bits, colour_order, heat_level, heat_height, heat_angle)
    trial_a, trial_b = [ta0, ta1], [tb0, tb1]
    rdx, rdi = swap_cross(dx), swap_in(di)

    w_in = kernel_call(
        functools.partial(weight_kernel, planes, half, True),
        [vm(2, planes, 6, half, columns)] * 2,
        [VM] * 4,
    )(couplings, ri[0], info0, info1)
    w_x = kernel_call(
        functools.partial(weight_kernel, planes, half, False),
        [vm(2, 2, 6, half, columns)] * 2,
        [VM] * 4,
    )(couplings, rx[0], info0, info1)

    assert OR_SWEEPS == 2
    for sweep in range(OR_SWEEPS):
        first = sweep == 0
        new_in, bi = [None] * 2, [None] * 2
        for u in range(2):
            new_in[u], bi[u] = kernel_call(
                functools.partial(relax_early, planes, half, first),
                [vm(3 * planes * half, columns), pair],
                [VM] * 6,
            )(info[u], w_in[u], sx[u], si[u], ri[u], a_in[u])
        for u in range(2):
            *a_x[u], sx[u] = kernel_call(
                functools.partial(relax_late, planes, half, first),
                [pair] * (1 + first),
                [VM] * (6 if first else 7),
                scratch=[] if first else [pair],
            )(info[u], w_in[u], w_x[u], sx[u], rx[u], new_in[u], *a_x[u])
            si[u], a_in[u] = bi[u], new_in[u]
            rx[u] = swap_cross(sx[u])
            ri[u] = swap_in(si[u])

    inner, outer, part, r_inner, r_outer = ([None] * 2 for _ in range(5))
    for u in range(2):
        inner[u], part[u] = kernel_call(
            functools.partial(heat_early, planes, half, u),
            [vm(EARLY * half + 8, columns), vm(half, columns)],
            [VM] * 9,
            scratch=[vm(3, half, columns)],
        )(info[u], beta[u], w_in[u], sx[u], si[u], ri[u], trial_a[u], trial_b[u], rdi)
        r_inner[u] = away(inner[u], u)
    energy = []
    for u in range(2):
        outer[u], *energy = kernel_call(
            functools.partial(heat_late, planes, half, u),
            [vm(LATE * half, columns), vm(count, 2) if u else vm(8, columns)],
            [VM] * (11 + u),
            scratch=[vm(3, half, columns)],
        )(
            info[u], beta[u], w_in[u], w_x[u], sx[u], rx[u],
            trial_a[u], trial_b[u], rdx, inner[u], part[u], *energy,
        )
        r_outer[u] = away(outer[u], u)

    parts = lax.all_to_all(energy[0], "gz", split_axis=0, concat_axis=0, tiled=True)
    (total,) = kernel_call(
        functools.partial(total_kernel, float(columns * rows * planes * count)), [vm(1, 2)], [VM]
    )(parts)
    r_total = [away(total, u) for u in range(2)]

    (spin_final,) = kernel_call(
        functools.partial(out_kernel, planes, half),
        [jax.ShapeDtypeStruct(spin_state.shape, F32)],
        [VM] * 10,
        out_specs=[ANY],
        scratch=[vm(*spin_state.shape), pltpu.SemaphoreType.DMA((2,))],
    )(info0, info1, *inner, *outer, *r_inner, *r_outer)
    (energies,) = kernel_call(
        functools.partial(energy_kernel, half), [vm(1, 2)], [VM] * 7
    )(info0, info1, total, *r_total, *r_inner)
    return spin_final, energies.reshape(-1)


def solution(mesh):
    return jax.shard_map(
        step,
        mesh=mesh,
        in_specs=(
            P(("group", "temp"), None, "gz", None, None),
            P(None, ("group", "gz"), None, None),
            P(("group", "temp")),
            P(("group", "temp")),
            P(("group", "temp"), "gz", None, None),
            P(("group", "temp"), "gz", None, None),
            P(("group", "temp"), "gz", None, None),
            P(("group", "temp")),
        ),
        out_specs=(P(("group", "temp"), None, "gz", None, None), P(("group", "temp"))),
        check_vma=False,
    )
```

```python
import functools

import jax
import jax.numpy as jnp
from jax import lax
from jax.experimental import pallas as pl
from jax.experimental.pallas import tpu as pltpu
from jax.sharding import PartitionSpec as P


F32 = jnp.float32
OR_SWEEPS = 2


VM = pl.BlockSpec(memory_space=pltpu.VMEM)
SM = pl.BlockSpec(memory_space=pltpu.SMEM)
ANY = pl.BlockSpec(memory_space=pl.ANY)
HBM = pl.BlockSpec(memory_space=pltpu.HBM)
PIECES = 9
EARLY = 15
LATE = 9


def vm(*shape, dtype=F32):
    return pltpu.VMEM(shape, dtype)


def kernel_call(body, outs, in_specs, out_specs=None, scratch=(), mib=24):
    return pl.pallas_call(
        body,
        out_shape=outs,
        in_specs=in_specs,
        out_specs=out_specs if out_specs is not None else [VM] * len(outs),
        scratch_shapes=list(scratch),
        compiler_params=pltpu.CompilerParams(vmem_limit_bytes=mib * 1024 * 1024),
    )


def in_hbm(value):
    return pltpu.with_memory_space_constraint(value, pltpu.HBM)


def core_index():
    return lax.rem(lax.axis_index("gz"), 2)


def slot_of(u):
    odd = lax.rem(lax.axis_index("temp"), 2)
    return 1 - odd if u == 0 else odd


def slot_replica(swap, u):
    return slot_of(u) ^ (swap[0] != 0).astype(jnp.int32)


def lane_even(rows, columns, offset):
    lane = lax.broadcasted_iota(jnp.int32, (rows, columns), 1)
    return ((lane + offset) & 1) == 0


def tile(ref, i, half):
    return ref[pl.ds(i * half, half), :]


def put(ref, i, value):
    half = value.shape[0]
    ref[pl.ds(i * half, half), :] = value


def folded(ref, index, half):
    return tuple(ref[(*index, pl.ds(s, half, stride=2), slice(None))] for s in (0, 1))


def folded_rows(ref, base, half):
    return tuple(ref[pl.ds(base + s, half, stride=2), :] for s in (0, 1))


def parity(info, half):
    columns = info.shape[-1]
    lane = lax.broadcasted_iota(jnp.int32, (half, columns), 1)
    return (lane & 1) == jnp.broadcast_to(info[0:1, :], (half, columns))


def at_plane(even, w):
    return even if w % 2 == 0 else jnp.logical_not(even)


def bond_copies(planes, coup, target, base, rows, side_in, sems):
    core = core_index()
    top = planes - 1
    at_top = 1 - core if side_in else core
    z = at_top * top
    return [
        pltpu.make_async_copy(coup.at[d, p], target.at[pl.ds(base + i * rows, rows), :], sems.at[i])
        for i, (d, p) in enumerate(((0, z), (1, z), (2, at_top * (top - 1)), (2, z)))
    ]


def bond_kernel(planes, coup, out, sems):
    copies = bond_copies(planes, coup, out, 0, coup.shape[2], False, sems)
    for copy in copies:
        copy.start()
    for copy in copies:
        copy.wait()


def load_kernel(planes, half, *refs):
    (swap_h, colour_h, beta_h, spin_h, coup_h) = refs[:5]
    (p0x, p0i, p1x, p1i, am0, am1, info0, info1, beta0, beta1) = refs[5:15]
    swap, colour, betas, spin, sems, bond_sems = refs[15:]
    core = core_index()
    columns = spin.shape[-1]
    rows = 2 * half
    top = planes - 1
    scalars = [
        pltpu.make_async_copy(swap_h, swap, sems.at[0]),
        pltpu.make_async_copy(colour_h, colour, sems.at[1]),
        pltpu.make_async_copy(beta_h, betas, sems.at[2]),
    ]
    spins = [
        pltpu.make_async_copy(spin_h.at[:, :, w + core * (top - 2 * w)], spin.at[w], sems.at[3 + w])
        for w in range(planes)
    ]
    bonds = bond_copies(planes, coup_h, p0i, PIECES * half, rows, True, bond_sems)
    for copy in scalars + spins + bonds:
        copy.start()
    for copy in scalars:
        copy.wait()
    reps, masks = [], []
    for u, info, beta in ((0, info0, beta0), (1, info1, beta1)):
        rep = slot_replica(swap, u)
        c = colour[rep] ^ core
        info[0:1, :] = jnp.full((1, columns), c, jnp.int32)
        info[1:2, :] = jnp.full((1, columns), (swap[1] != 0).astype(jnp.int32), jnp.int32)
        beta[...] = jnp.full(beta.shape, betas[rep], F32)
        reps.append(rep)
        masks.append(lane_even(half, columns, c))
    for w in range(planes):
        spins[w].wait()
        for u, sx, si, am in ((0, p0x, p0i, am0), (1, p1x, p1i, am1)):
            m = at_plane(masks[u], w)
            for k in range(3):
                even, odd = folded(spin, (w, reps[u], k), half)
                a = jnp.where(m, even, odd)
                b = jnp.where(m, odd, even)
                if w == 0:
                    put(sx, k, b)
                    put(sx, 6 + k, a)
                elif w == 1:
                    put(sx, 3 + k, b)
                    put(am, k, a)
                elif w == planes - 2:
                    put(si, 3 + k, b)
                    put(am, 3 + k, a)
                else:
                    put(si, k, b)
                    put(si, 6 + k, a)
    for copy in bonds:
        copy.wait()


def weight_kernel(planes, half, in_chip, *refs):
    coup, sent_ref, info0, info1, weights0, weights1 = refs
    core = core_index()
    top = planes - 1
    rows = 2 * half
    first = core == 0

    def sent(i):
        return folded_rows(sent_ref, (PIECES * half if in_chip else 0) + i * rows, half)

    def zbond(m):
        if m in (-1, planes + 1):
            return sent(2)
        if m in (0, planes):
            ours, theirs = folded(coup, (2, top), half), sent(3)
            mine = first if m == planes else jnp.logical_not(first)
            return tuple(jnp.where(mine, o, t) for o, t in zip(ours, theirs))
        return folded(coup, (2, (m - 1) + core * (top - 2 * m + 1)), half)

    span = range(1, planes + 1) if in_chip else range(-1, 1)
    below = zbond(span[0])
    for i, w in enumerate(span):
        above = zbond(w + 1)
        if w in (-1, planes):
            jx, jy = sent(0), sent(1)
        else:
            z = w + core * (top - 2 * w)
            jx, jy = folded(coup, (0, z), half), folded(coup, (1, z), half)
        up_odd = pltpu.roll(jy[1], 1, 0)
        for info, weights in ((info0, weights0), (info1, weights1)):
            even = parity(info, half)
            for a in (0, 1):
                if a == 1 and w in (-1, planes):
                    continue
                m = at_plane(even, w + a)
                weights[a, i, 0] = jnp.where(m, jx[0], jx[1])
                weights[a, i, 1] = pltpu.roll(jnp.where(m, jx[1], jx[0]), 1, 1)
                weights[a, i, 2] = jy[0]
                weights[a, i, 3] = jnp.where(m, up_odd, jy[1])
                weights[a, i, 4] = jnp.where(m, above[0], above[1])
                weights[a, i, 5] = jnp.where(m, below[0], below[1])
        below = above


def field(get, weight, a, even, w):
    total = []
    m = at_plane(even, w + a)
    for k in range(3):
        o = get(w, k)
        half, columns = o.shape
        side = jnp.where(m, pltpu.roll(o, 1, 0), pltpu.roll(o, half - 1, 0))
        h = weight(a, w, 0) * pltpu.roll(o, columns - 1, 1)
        h = h + weight(a, w, 1) * pltpu.roll(o, 1, 1)
        h = h + weight(a, w, 2) * o
        h = h + weight(a, w, 3) * side
        h = h + weight(a, w, 4) * get(w + 1, k)
        h = h + weight(a, w, 5) * get(w - 1, k)
        total.append(h)
    return total


def weight_of(w_in, w_x):
    return lambda a, w, i: w_in[a, w - 1, i] if w > 0 else w_x[a, w + 1, i]


def dot3(a, b):
    return a[0] * b[0] + a[1] * b[1] + a[2] * b[2]


def reflect(s, h):
    f = 2.0 * dot3(s, h) / jnp.maximum(dot3(h, h), 0.01)
    return [f * h[k] - s[k] for k in range(3)]


def second_planes(planes, half, sx, si, rx, ri):
    def get(w, k):
        if w < 0:
            return tile(rx, 3 * (-1 - w) + k, half)
        if w < 2:
            return tile(sx, 3 * w + k, half)
        if w < planes:
            return tile(si, 3 * (planes - 1 - w) + k, half)
        return tile(ri, 3 * (w - planes) + k, half)

    return get


def relax_early(planes, half, first, *refs):
    info, w_in, sx, si, ri, a_old, a_new, bi = refs
    even = parity(info, half)
    weight = weight_of(w_in, None)
    get_b = second_planes(planes, half, sx, si, None, ri)

    def get_a(w, k):
        if not first:
            return tile(a_old, 3 * (w - 1) + k, half)
        if w == planes - 1:
            return tile(si, 6 + k, half)
        if w == planes:
            return tile(ri, 6 + k, half)
        return tile(a_old, 3 * (w - 1) + k, half)

    for w in range(1, planes + 1):
        h = field(get_b, weight, 0, even, w)
        new = reflect([get_a(w, k) for k in range(3)], h)
        for k in range(3):
            put(a_new, 3 * (w - 1) + k, new[k])
    for w in range(2, planes):
        h = field(lambda v, k: tile(a_new, 3 * (v - 1) + k, half), weight, 1, even, w)
        new = reflect([get_b(w, k) for k in range(3)], h)
        for k in range(3):
            put(bi, 3 * (planes - 1 - w) + k, new[k])


def relax_late(planes, half, first, *refs):
    info, w_in, w_x, sx, rx, a_in = refs[:6]
    a_old, a_new, bx = (None, *refs[6:]) if first else (refs[6], refs[8], refs[7])
    even = parity(info, half)
    weight = weight_of(w_in, w_x)
    get_b = second_planes(planes, half, sx, None, rx, None)

    def get_a(w, k):
        if not first:
            return tile(a_old, 3 * (w + 1) + k, half)
        return tile(rx if w < 0 else sx, 6 + k, half)

    for w in (-1, 0):
        h = field(get_b, weight, 0, even, w)
        new = reflect([get_a(w, k) for k in range(3)], h)
        for k in range(3):
            put(a_new, 3 * (w + 1) + k, new[k])

    def get_new(w, k):
        return tile(a_new, 3 * (w + 1) + k, half) if w < 1 else tile(a_in, 3 * (w - 1) + k, half)

    for w in (0, 1):
        h = field(get_new, weight, 1, even, w)
        new = reflect([get_b(w, k) for k in range(3)], h)
        for k in range(3):
            put(bx, 3 * w + k, new[k])


SIN = (1.0, -1 / 6, 1 / 120, -1 / 5040, 1 / 362880, -1 / 39916800, 1 / 6227020800)
COS = (1.0, -1 / 2, 1 / 24, -1 / 720, 1 / 40320, -1 / 3628800, 1 / 479001600, -1 / 87178291200)


def series(coefficients, y):
    total = coefficients[-1]
    for value in coefficients[-2::-1]:
        total = total * y + value
    return total


def trial(height, angle):
    t = 0.5 * angle
    y = t * t
    s = t * series(SIN, y)
    c = series(COS, y)
    q = jnp.sqrt(jnp.maximum(1.0 - height * height, 0.0))
    return q * (1.0 - 2.0 * (s * s)), q * (2.0 * (s * c))


def trial_kernel(planes, half, swap, colour, level, height, angle, ta0, tb0, ta1, tb1, dx, di):
    core = core_index()
    columns = level.shape[-1]
    for u, ta, tb in ((0, ta0, tb0), (1, ta1, tb1)):
        rep = slot_replica(swap, u)
        c = colour[rep]
        for w in range(planes):
            z = w + core * (planes - 1 - 2 * w)
            m = lane_even(half, columns, z + c)
            a, b = [], []
            for ref in (level, height, angle):
                even, odd = folded(ref, (rep, z), half)
                a.append(jnp.where(m, even, odd))
                b.append(jnp.where(m, odd, even))
            if w == 0 or w == planes - 1:
                for i in range(3):
                    put(dx if w == 0 else di, 3 * u + i, a[i])
            for t, (lev, hei, ang) in ((ta, a), (tb, b)):
                ux, uy = trial(hei, ang)
                t[w, 0], t[w, 1], t[w, 2], t[w, 3] = ux, uy, hei, lev


def trial_of(t, w):
    return [t[w, k] for k in range(3)], t[w, 3]


def trial_sent(draws, u, half):
    level, height, angle = (tile(draws, 3 * u + i, half) for i in range(3))
    ux, uy = trial(height, angle)
    return [ux, uy, height], level


def heated(h, u, level, beta):
    m = jnp.maximum(dot3(h, h), 0.01)
    inverse = lax.rsqrt(m)
    e = [h[k] * inverse for k in range(3)]
    reach = beta * (m * inverse)
    c = 1.0 + jnp.log(1.0 + level * (jnp.exp(-2.0 * reach) - 1.0)) / reach
    along = dot3(u, e)
    t = [u[k] - along * e[k] for k in range(3)]
    f = jnp.sqrt(jnp.maximum(1.0 - c * c, 0.0)) * lax.rsqrt(jnp.maximum(dot3(t, t), 0.0001))
    return [c * e[k] + f * t[k] for k in range(3)]


def heat_early(planes, half, u, *refs):
    info, betas, w_in, sx, si, ri, ta, tb, rdi, out, e_part, halo = refs
    even = parity(info, half)
    columns = info.shape[-1]
    beta = jnp.broadcast_to(betas[0:1, :], (half, columns))
    weight = weight_of(w_in, None)
    get_b = second_planes(planes, half, sx, si, None, ri)

    def get_a(w, k):
        return halo[k] if w == planes else tile(out, 3 * (w - 1) + k, half)

    for w in range(1, planes + 1):
        h = field(get_b, weight, 0, even, w)
        draw = trial_of(ta, w) if w < planes else trial_sent(rdi, u, half)
        new = heated(h, *draw, beta)
        for k in range(3):
            if w == planes:
                halo[k] = new[k]
            else:
                put(out, 3 * (w - 1) + k, new[k])
    energy = None
    for w in range(2, planes):
        h = field(get_a, weight, 1, even, w)
        new = heated(h, *trial_of(tb, w), beta)
        for k in range(3):
            put(out, 9 + 3 * (w - 2) + k, new[k])
        term = dot3(new, h)
        energy = term if energy is None else energy + term
    e_part[...] = energy
    out[pl.ds(EARLY * half, 8), :] = info[...].astype(F32)


def heat_late(planes, half, u, *refs):
    info, betas, w_in, w_x, sx, rx, ta, tb, rdx, inner, e_part = refs[:11]
    if u == 0:
        out, e_out, halo = refs[11:]
    else:
        e_other, out, e_out, halo = refs[11:]
    even = parity(info, half)
    columns = info.shape[-1]
    beta = jnp.broadcast_to(betas[0:1, :], (half, columns))
    weight = weight_of(w_in, w_x)
    get_b = second_planes(planes, half, sx, None, rx, None)

    def get_a(w, k):
        if w < 0:
            return halo[k]
        return tile(out, k, half) if w == 0 else tile(inner, 3 * (w - 1) + k, half)

    for w in (-1, 0):
        h = field(get_b, weight, 0, even, w)
        draw = trial_of(ta, w) if w >= 0 else trial_sent(rdx, u, half)
        new = heated(h, *draw, beta)
        for k in range(3):
            if w < 0:
                halo[k] = new[k]
            else:
                put(out, k, new[k])
    energy = e_part[...]
    for w in (0, 1):
        h = field(get_a, weight, 1, even, w)
        new = heated(h, *trial_of(tb, w), beta)
        for k in range(3):
            put(out, 3 + 3 * w + k, new[k])
        energy = energy + dot3(new, h)
    mine = jnp.full(e_out.shape, -jnp.sum(energy), F32)
    if u == 1:
        lane = lax.broadcasted_iota(jnp.int32, e_out.shape, 1)
        other = jnp.broadcast_to(e_other[0:1, : e_out.shape[1]], e_out.shape)
        mine = jnp.where(lane == 0, other, mine)
    e_out[...] = mine


def total_kernel(sites, parts, total):
    total[...] = jnp.sum(parts[...], axis=0, keepdims=True) / sites


def exchanged(u, info, note):
    place = lax.axis_index("temp")
    upper = slot_of(u) == 1
    ours = jnp.max(info[1:2, :]) > 0
    theirs = jnp.max(note[1:2, :]) > 0.5
    inside = jnp.where(upper, place != lax.axis_size("temp") - 1, place != 0)
    return jnp.logical_and(jnp.where(upper, ours, theirs), inside)


def out_kernel(planes, half, *refs):
    info0, info1, i0, i1, o0, o1, ri0, ri1, ro0, ro1, out_h, taken, out, sems = refs
    core = core_index()
    columns = out.shape[-1]
    pushes = []
    for u, info, own, other in ((0, info0, (i0, o0), (ri0, ro0)), (1, info1, (i1, o1), (ri1, ro1))):
        note = ri0[pl.ds(EARLY * half, 8), :] if u == 0 else ri1[pl.ds(EARLY * half, 8), :]
        take = exchanged(u, info, note)
        taken[u : u + 1, :] = jnp.full((1, columns), take.astype(jnp.int32), jnp.int32)

        def write(early, late, parities):
            even = (lax.broadcasted_iota(jnp.int32, (half, columns), 1) & 1) == jnp.broadcast_to(
                parities, (half, columns)
            )
            for w in range(planes):
                z = w + core * (planes - 1 - 2 * w)
                m = at_plane(even, w)
                for k in range(3):
                    a = tile(late, k, half) if w == 0 else tile(early, 3 * (w - 1) + k, half)
                    b = tile(late, 3 + 3 * w + k, half) if w < 2 else tile(early, 3 + 3 * w + k, half)
                    out[u, k, z, pl.ds(0, half, stride=2), :] = jnp.where(m, a, b)
                    out[u, k, z, pl.ds(1, half, stride=2), :] = jnp.where(m, b, a)

        @pl.when(take)
        def _():
            write(*other, note[0:1, :].astype(jnp.int32))

        @pl.when(jnp.logical_not(take))
        def _():
            write(*own, info[0:1, :])

        push = pltpu.make_async_copy(out.at[u], out_h.at[slot_of(u)], sems.at[u])
        push.start()
        pushes.append(push)
    for push in pushes:
        push.wait()


def energy_kernel(taken, total, r0, r1, energies_h, energies, sem):
    final = [
        jnp.where(taken[u : u + 1, u : u + 1] > 0, r[:, u : u + 1], total[:, u : u + 1])
        for u, r in ((0, r0), (1, r1))
    ]
    lane = lax.broadcasted_iota(jnp.int32, energies.shape, 1)
    energies[...] = jnp.where(
        lane == slot_of(0),
        jnp.broadcast_to(final[0], energies.shape),
        jnp.broadcast_to(final[1], energies.shape),
    )
    copy = pltpu.make_async_copy(energies, energies_h, sem)
    copy.start()
    copy.wait()


def step(
    spin_state, couplings, inverse_temps, colour_order, heat_level, heat_height, heat_angle, swap_bits
):
    replicas, _, planes, rows, columns = spin_state.shape
    half = rows // 2
    count = lax.axis_size("gz")
    temps = lax.axis_size("temp")
    assert replicas == 2 and planes == 4 and rows % 2 == 0 and columns % 2 == 0
    assert count % 2 == 0 and temps % 2 == 0
    in_chip = [(i, i ^ 1) for i in range(count)]
    cross = [(i, (i + (1 if i % 2 else -1)) % count) for i in range(count)]
    partners = (
        [(i, i ^ 1) for i in range(temps)],
        [(i, (i + (1 if i % 2 else -1)) % temps) for i in range(temps)],
    )

    def swap_in(value):
        return lax.ppermute(value, "gz", in_chip)

    def swap_cross(value):
        return lax.ppermute(value, "gz", cross)

    def away(value, u):
        return lax.ppermute(value, "temp", partners[u])

    spins = PIECES * half
    pair = vm(6 * half, columns)
    (bonds,) = kernel_call(
        functools.partial(bond_kernel, planes),
        [vm(4 * rows, columns)],
        [HBM],
        scratch=[pltpu.SemaphoreType.DMA((4,))],
    )(in_hbm(couplings))
    r_bonds = swap_cross(bonds)
    p0x, p0i, p1x, p1i, am0, am1, info0, info1, beta0, beta1 = kernel_call(
        functools.partial(load_kernel, planes, half),
        [vm(spins, columns), vm(spins + 4 * rows, columns)]
        + [vm(spins, columns)] * 2
        + [pair] * 2
        + [vm(8, columns, dtype=jnp.int32)] * 2
        + [vm(8, columns)] * 2,
        [HBM] * 5,
        scratch=[
            pltpu.SMEM((replicas,), jnp.int32),
            pltpu.SMEM((replicas,), jnp.int32),
            pltpu.SMEM((replicas,), F32),
            vm(planes, replicas, 3, rows, columns),
            pltpu.SemaphoreType.DMA((3 + planes,)),
            pltpu.SemaphoreType.DMA((4,)),
        ],
    )(*(in_hbm(v) for v in (swap_bits, colour_order, inverse_temps, spin_state, couplings)))
    info, beta = [info0, info1], [beta0, beta1]
    sx, si, a_in, a_x = [p0x, p1x], [p0i, p1i], [am0, am1], [[], []]
    rx = [swap_cross(sx[u]) for u in range(2)]
    ri = [swap_in(si[u]) for u in range(2)]

    ta0, tb0, ta1, tb1, dx, di = kernel_call(
        functools.partial(trial_kernel, planes, half),
        [vm(planes, 4, half, columns)] * 4 + [pair] * 2,
        [SM, SM, VM, VM, VM],
    )(swap_bits, colour_order, heat_level, heat_height, heat_angle)
    trial_a, trial_b = [ta0, ta1], [tb0, tb1]
    rdx, rdi = swap_cross(dx), swap_in(di)

    w_in = kernel_call(
        functools.partial(weight_kernel, planes, half, True),
        [vm(2, planes, 6, half, columns)] * 2,
        [VM] * 4,
    )(couplings, ri[0], info0, info1)
    w_x = kernel_call(
        functools.partial(weight_kernel, planes, half, False),
        [vm(2, 2, 6, half, columns)] * 2,
        [VM] * 4,
    )(couplings, r_bonds, info0, info1)

    assert OR_SWEEPS == 2
    for sweep in range(OR_SWEEPS):
        first = sweep == 0
        new_in, bi = [None] * 2, [None] * 2
        for u in range(2):
            new_in[u], bi[u] = kernel_call(
                functools.partial(relax_early, planes, half, first),
                [vm(3 * planes * half, columns), pair],
                [VM] * 6,
            )(info[u], w_in[u], sx[u], si[u], ri[u], a_in[u])
        for u in range(2):
            *a_x[u], sx[u] = kernel_call(
                functools.partial(relax_late, planes, half, first),
                [pair] * (1 + first),
                [VM] * (6 if first else 7),
                scratch=[] if first else [pair],
            )(info[u], w_in[u], w_x[u], sx[u], rx[u], new_in[u], *a_x[u])
            si[u], a_in[u] = bi[u], new_in[u]
            rx[u] = swap_cross(sx[u])
            ri[u] = swap_in(si[u])

    inner, outer, part, r_inner, r_outer = ([None] * 2 for _ in range(5))
    for u in range(2):
        inner[u], part[u] = kernel_call(
            functools.partial(heat_early, planes, half, u),
            [vm(EARLY * half + 8, columns), vm(half, columns)],
            [VM] * 9,
            scratch=[vm(3, half, columns)],
        )(info[u], beta[u], w_in[u], sx[u], si[u], ri[u], trial_a[u], trial_b[u], rdi)
        r_inner[u] = away(inner[u], u)
    energy = []
    for u in range(2):
        outer[u], *energy = kernel_call(
            functools.partial(heat_late, planes, half, u),
            [vm(LATE * half, columns), vm(count, 2) if u else vm(8, columns)],
            [VM] * (11 + u),
            scratch=[vm(3, half, columns)],
        )(
            info[u], beta[u], w_in[u], w_x[u], sx[u], rx[u],
            trial_a[u], trial_b[u], rdx, inner[u], part[u], *energy,
        )
        r_outer[u] = away(outer[u], u)

    parts = lax.all_to_all(energy[0], "gz", split_axis=0, concat_axis=0, tiled=True)
    (total,) = kernel_call(
        functools.partial(total_kernel, float(columns * rows * planes * count)), [vm(1, 2)], [VM]
    )(parts)
    r_total = [away(total, u) for u in range(2)]

    spin_final, taken = kernel_call(
        functools.partial(out_kernel, planes, half),
        [jax.ShapeDtypeStruct(spin_state.shape, F32), vm(8, columns, dtype=jnp.int32)],
        [VM] * 10,
        out_specs=[HBM, VM],
        scratch=[vm(*spin_state.shape), pltpu.SemaphoreType.DMA((2,))],
    )(info0, info1, *inner, *outer, *r_inner, *r_outer)
    (energies,) = kernel_call(
        energy_kernel,
        [jax.ShapeDtypeStruct((1, 2), F32)],
        [VM] * 4,
        out_specs=[HBM],
        scratch=[vm(1, 2), pltpu.SemaphoreType.DMA(())],
    )(taken, total, *r_total)
    return spin_final, energies.reshape(-1)


def solution(mesh):
    return jax.shard_map(
        step,
        mesh=mesh,
        in_specs=(
            P(("group", "temp"), None, "gz", None, None),
            P(None, ("group", "gz"), None, None),
            P(("group", "temp")),
            P(("group", "temp")),
            P(("group", "temp"), "gz", None, None),
            P(("group", "temp"), "gz", None, None),
            P(("group", "temp"), "gz", None, None),
            P(("group", "temp")),
        ),
        out_specs=(P(("group", "temp"), None, "gz", None, None), P(("group", "temp"))),
        check_vma=False,
    )
```

```python
import functools

import jax
import jax.numpy as jnp
from jax import lax
from jax.experimental import pallas as pl
from jax.experimental.pallas import tpu as pltpu
from jax.sharding import PartitionSpec as P


F32 = jnp.float32
OR_SWEEPS = 2


VM = pl.BlockSpec(memory_space=pltpu.VMEM)
SM = pl.BlockSpec(memory_space=pltpu.SMEM)
ANY = pl.BlockSpec(memory_space=pl.ANY)
HBM = pl.BlockSpec(memory_space=pltpu.HBM)
PIECES = 9
EARLY = 15
LATE = 9


def vm(*shape, dtype=F32):
    return pltpu.VMEM(shape, dtype)


def kernel_call(body, outs, in_specs, out_specs=None, scratch=(), mib=24):
    return pl.pallas_call(
        body,
        out_shape=outs,
        in_specs=in_specs,
        out_specs=out_specs if out_specs is not None else [VM] * len(outs),
        scratch_shapes=list(scratch),
        compiler_params=pltpu.CompilerParams(vmem_limit_bytes=mib * 1024 * 1024),
    )


def in_hbm(value):
    return pltpu.with_memory_space_constraint(value, pltpu.HBM)


def core_index():
    return lax.rem(lax.axis_index("gz"), 2)


def slot_of(u):
    odd = lax.rem(lax.axis_index("temp"), 2)
    return 1 - odd if u == 0 else odd


def slot_replica(swap, u):
    return slot_of(u) ^ (swap[0] != 0).astype(jnp.int32)


def lane_even(rows, columns, offset):
    lane = lax.broadcasted_iota(jnp.int32, (rows, columns), 1)
    return ((lane + offset) & 1) == 0


def tile(ref, i, half):
    return ref[pl.ds(i * half, half), :]


def put(ref, i, value):
    half = value.shape[0]
    ref[pl.ds(i * half, half), :] = value


def folded(ref, index, half):
    return tuple(ref[(*index, pl.ds(s, half, stride=2), slice(None))] for s in (0, 1))


def folded_rows(ref, base, half):
    return tuple(ref[pl.ds(base + s, half, stride=2), :] for s in (0, 1))


def parity(info, half):
    columns = info.shape[-1]
    lane = lax.broadcasted_iota(jnp.int32, (half, columns), 1)
    return (lane & 1) == jnp.broadcast_to(info[0:1, :], (half, columns))


def at_plane(even, w):
    return even if w % 2 == 0 else jnp.logical_not(even)


def bond_copies(planes, coup, target, base, rows, side_in, sems):
    core = core_index()
    top = planes - 1
    at_top = 1 - core if side_in else core
    z = at_top * top
    return [
        pltpu.make_async_copy(coup.at[d, p], target.at[pl.ds(base + i * rows, rows), :], sems.at[i])
        for i, (d, p) in enumerate(((0, z), (1, z), (2, at_top * (top - 1)), (2, z)))
    ]


def load_kernel(planes, half, *refs):
    (swap_h, colour_h, beta_h, spin_h, coup_h) = refs[:5]
    p0x, p1x, pi, am0, am1, info0, info1, beta0, beta1 = refs[5:14]
    swap, colour, betas, spin, sems, bond_sems = refs[14:]
    core = core_index()
    columns = spin.shape[-1]
    rows = 2 * half
    top = planes - 1
    scalars = [
        pltpu.make_async_copy(swap_h, swap, sems.at[0]),
        pltpu.make_async_copy(colour_h, colour, sems.at[1]),
        pltpu.make_async_copy(beta_h, betas, sems.at[2]),
    ]
    spins = [
        pltpu.make_async_copy(spin_h.at[:, :, w + core * (top - 2 * w)], spin.at[w], sems.at[3 + w])
        for w in range(planes)
    ]
    bonds = bond_copies(planes, coup_h, p0x, PIECES * half, rows, False, bond_sems.at[0])
    bonds += bond_copies(planes, coup_h, pi, 2 * PIECES * half, rows, True, bond_sems.at[1])
    for copy in scalars + spins + bonds:
        copy.start()
    for copy in scalars:
        copy.wait()
    reps, masks = [], []
    for u, info, beta in ((0, info0, beta0), (1, info1, beta1)):
        rep = slot_replica(swap, u)
        c = colour[rep] ^ core
        info[0:1, :] = jnp.full((1, columns), c, jnp.int32)
        info[1:2, :] = jnp.full((1, columns), (swap[1] != 0).astype(jnp.int32), jnp.int32)
        beta[...] = jnp.full(beta.shape, betas[rep], F32)
        reps.append(rep)
        masks.append(lane_even(half, columns, c))
    for w in range(planes):
        spins[w].wait()
        for u, sx, am in ((0, p0x, am0), (1, p1x, am1)):
            base = PIECES * u
            m = at_plane(masks[u], w)
            for k in range(3):
                even, odd = folded(spin, (w, reps[u], k), half)
                a = jnp.where(m, even, odd)
                b = jnp.where(m, odd, even)
                if w == 0:
                    put(sx, k, b)
                    put(sx, 6 + k, a)
                elif w == 1:
                    put(sx, 3 + k, b)
                    put(am, k, a)
                elif w == planes - 2:
                    put(pi, base + 3 + k, b)
                    put(am, 3 + k, a)
                else:
                    put(pi, base + k, b)
                    put(pi, base + 6 + k, a)
    for copy in bonds:
        copy.wait()


def weight_kernel(planes, half, in_chip, *refs):
    coup, sent_ref, info0, info1, weights0, weights1 = refs
    core = core_index()
    top = planes - 1
    rows = 2 * half
    first = core == 0

    def sent(i):
        return folded_rows(sent_ref, (2 if in_chip else 1) * PIECES * half + i * rows, half)

    def zbond(m):
        if m in (-1, planes + 1):
            return sent(2)
        if m in (0, planes):
            ours, theirs = folded(coup, (2, top), half), sent(3)
            mine = first if m == planes else jnp.logical_not(first)
            return tuple(jnp.where(mine, o, t) for o, t in zip(ours, theirs))
        return folded(coup, (2, (m - 1) + core * (top - 2 * m + 1)), half)

    span = range(1, planes + 1) if in_chip else range(-1, 1)
    below = zbond(span[0])
    for i, w in enumerate(span):
        above = zbond(w + 1)
        if w in (-1, planes):
            jx, jy = sent(0), sent(1)
        else:
            z = w + core * (top - 2 * w)
            jx, jy = folded(coup, (0, z), half), folded(coup, (1, z), half)
        up_odd = pltpu.roll(jy[1], 1, 0)
        for info, weights in ((info0, weights0), (info1, weights1)):
            even = parity(info, half)
            for a in (0, 1):
                if a == 1 and w in (-1, planes):
                    continue
                m = at_plane(even, w + a)
                weights[a, i, 0] = jnp.where(m, jx[0], jx[1])
                weights[a, i, 1] = pltpu.roll(jnp.where(m, jx[1], jx[0]), 1, 1)
                weights[a, i, 2] = jy[0]
                weights[a, i, 3] = jnp.where(m, up_odd, jy[1])
                weights[a, i, 4] = jnp.where(m, above[0], above[1])
                weights[a, i, 5] = jnp.where(m, below[0], below[1])
        below = above


def field(get, weight, a, even, w):
    total = []
    m = at_plane(even, w + a)
    for k in range(3):
        o = get(w, k)
        half, columns = o.shape
        side = jnp.where(m, pltpu.roll(o, 1, 0), pltpu.roll(o, half - 1, 0))
        h = weight(a, w, 0) * pltpu.roll(o, columns - 1, 1)
        h = h + weight(a, w, 1) * pltpu.roll(o, 1, 1)
        h = h + weight(a, w, 2) * o
        h = h + weight(a, w, 3) * side
        h = h + weight(a, w, 4) * get(w + 1, k)
        h = h + weight(a, w, 5) * get(w - 1, k)
        total.append(h)
    return total


def weight_of(w_in, w_x):
    return lambda a, w, i: w_in[a, w - 1, i] if w > 0 else w_x[a, w + 1, i]


def dot3(a, b):
    return a[0] * b[0] + a[1] * b[1] + a[2] * b[2]


def reflect(s, h):
    f = 2.0 * dot3(s, h) / jnp.maximum(dot3(h, h), 0.01)
    return [f * h[k] - s[k] for k in range(3)]


def second_planes(planes, half, sx, si, rx, ri, own=0, sent=0):
    def get(w, k):
        if w < 0:
            return tile(rx, 3 * (-1 - w) + k, half)
        if w < 2:
            return tile(sx, 3 * w + k, half)
        if w < planes:
            return tile(si, own + 3 * (planes - 1 - w) + k, half)
        return tile(ri, sent + 3 * (w - planes) + k, half)

    return get


def relax_early(planes, half, first, u, *refs):
    info, w_in, sx, si, ri, a_old = refs[:6]
    a_new, bi = refs[-2:]
    offset = (PIECES if first else 6) * u
    even = parity(info, half)
    weight = weight_of(w_in, None)
    get_b = second_planes(planes, half, sx, si, None, ri, offset, offset)
    if u == 1:
        bi[pl.ds(0, 6 * half), :] = refs[6][...]

    def get_a(w, k):
        if not first:
            return tile(a_old, 3 * (w - 1) + k, half)
        if w == planes - 1:
            return tile(si, offset + 6 + k, half)
        if w == planes:
            return tile(ri, offset + 6 + k, half)
        return tile(a_old, 3 * (w - 1) + k, half)

    for w in range(1, planes + 1):
        h = field(get_b, weight, 0, even, w)
        new = reflect([get_a(w, k) for k in range(3)], h)
        for k in range(3):
            put(a_new, 3 * (w - 1) + k, new[k])
    for w in range(2, planes):
        h = field(lambda v, k: tile(a_new, 3 * (v - 1) + k, half), weight, 1, even, w)
        new = reflect([get_b(w, k) for k in range(3)], h)
        for k in range(3):
            put(bi, 6 * u + 3 * (planes - 1 - w) + k, new[k])


def relax_late(planes, half, first, *refs):
    info, w_in, w_x, sx, rx, a_in = refs[:6]
    a_old, a_new, bx = (None, *refs[6:]) if first else (refs[6], refs[8], refs[7])
    even = parity(info, half)
    weight = weight_of(w_in, w_x)
    get_b = second_planes(planes, half, sx, None, rx, None)

    def get_a(w, k):
        if not first:
            return tile(a_old, 3 * (w + 1) + k, half)
        return tile(rx if w < 0 else sx, 6 + k, half)

    for w in (-1, 0):
        h = field(get_b, weight, 0, even, w)
        new = reflect([get_a(w, k) for k in range(3)], h)
        for k in range(3):
            put(a_new, 3 * (w + 1) + k, new[k])

    def get_new(w, k):
        return tile(a_new, 3 * (w + 1) + k, half) if w < 1 else tile(a_in, 3 * (w - 1) + k, half)

    for w in (0, 1):
        h = field(get_new, weight, 1, even, w)
        new = reflect([get_b(w, k) for k in range(3)], h)
        for k in range(3):
            put(bx, 3 * w + k, new[k])


SIN = (1.0, -1 / 6, 1 / 120, -1 / 5040, 1 / 362880, -1 / 39916800, 1 / 6227020800)
COS = (1.0, -1 / 2, 1 / 24, -1 / 720, 1 / 40320, -1 / 3628800, 1 / 479001600, -1 / 87178291200)


def series(coefficients, y):
    total = coefficients[-1]
    for value in coefficients[-2::-1]:
        total = total * y + value
    return total


def trial(height, angle):
    t = 0.5 * angle
    y = t * t
    s = t * series(SIN, y)
    c = series(COS, y)
    q = jnp.sqrt(jnp.maximum(1.0 - height * height, 0.0))
    return q * (1.0 - 2.0 * (s * s)), q * (2.0 * (s * c))


def trial_kernel(planes, half, swap, colour, level, height, angle, ta0, tb0, ta1, tb1, dx, di):
    core = core_index()
    columns = level.shape[-1]
    for u, ta, tb in ((0, ta0, tb0), (1, ta1, tb1)):
        rep = slot_replica(swap, u)
        c = colour[rep]
        for w in range(planes):
            z = w + core * (planes - 1 - 2 * w)
            m = lane_even(half, columns, z + c)
            a, b = [], []
            for ref in (level, height, angle):
                even, odd = folded(ref, (rep, z), half)
                a.append(jnp.where(m, even, odd))
                b.append(jnp.where(m, odd, even))
            if w == 0 or w == planes - 1:
                for i in range(3):
                    put(dx if w == 0 else di, 3 * u + i, a[i])
            for t, (lev, hei, ang) in ((ta, a), (tb, b)):
                ux, uy = trial(hei, ang)
                t[w, 0], t[w, 1], t[w, 2], t[w, 3] = ux, uy, hei, lev


def trial_of(t, w):
    return [t[w, k] for k in range(3)], t[w, 3]


def trial_sent(draws, u, half):
    level, height, angle = (tile(draws, 3 * u + i, half) for i in range(3))
    ux, uy = trial(height, angle)
    return [ux, uy, height], level


def heated(h, u, level, beta):
    m = jnp.maximum(dot3(h, h), 0.01)
    inverse = lax.rsqrt(m)
    e = [h[k] * inverse for k in range(3)]
    reach = beta * (m * inverse)
    c = 1.0 + jnp.log(1.0 + level * (jnp.exp(-2.0 * reach) - 1.0)) / reach
    along = dot3(u, e)
    t = [u[k] - along * e[k] for k in range(3)]
    f = jnp.sqrt(jnp.maximum(1.0 - c * c, 0.0)) * lax.rsqrt(jnp.maximum(dot3(t, t), 0.0001))
    return [c * e[k] + f * t[k] for k in range(3)]


def heat_early(planes, half, u, *refs):
    info, betas, w_in, sx, si, ri, ta, tb, rdi, out, e_part, halo = refs
    even = parity(info, half)
    columns = info.shape[-1]
    beta = jnp.broadcast_to(betas[0:1, :], (half, columns))
    weight = weight_of(w_in, None)
    get_b = second_planes(planes, half, sx, si, None, ri, 6 * u, 6 * u)

    def get_a(w, k):
        return halo[k] if w == planes else tile(out, 3 * (w - 1) + k, half)

    for w in range(1, planes + 1):
        h = field(get_b, weight, 0, even, w)
        draw = trial_of(ta, w) if w < planes else trial_sent(rdi, u, half)
        new = heated(h, *draw, beta)
        for k in range(3):
            if w == planes:
                halo[k] = new[k]
            else:
                put(out, 3 * (w - 1) + k, new[k])
    energy = None
    for w in range(2, planes):
        h = field(get_a, weight, 1, even, w)
        new = heated(h, *trial_of(tb, w), beta)
        for k in range(3):
            put(out, 9 + 3 * (w - 2) + k, new[k])
        term = dot3(new, h)
        energy = term if energy is None else energy + term
    e_part[...] = energy
    out[pl.ds(EARLY * half, 8), :] = info[...].astype(F32)


def heat_late(planes, half, u, *refs):
    info, betas, w_in, w_x, sx, rx, ta, tb, rdx, inner, e_part = refs[:11]
    if u == 0:
        out, e_out, halo = refs[11:]
    else:
        e_other, out, e_out, halo = refs[11:]
    even = parity(info, half)
    columns = info.shape[-1]
    beta = jnp.broadcast_to(betas[0:1, :], (half, columns))
    weight = weight_of(w_in, w_x)
    get_b = second_planes(planes, half, sx, None, rx, None)

    def get_a(w, k):
        if w < 0:
            return halo[k]
        return tile(out, k, half) if w == 0 else tile(inner, 3 * (w - 1) + k, half)

    for w in (-1, 0):
        h = field(get_b, weight, 0, even, w)
        draw = trial_of(ta, w) if w >= 0 else trial_sent(rdx, u, half)
        new = heated(h, *draw, beta)
        for k in range(3):
            if w < 0:
                halo[k] = new[k]
            else:
                put(out, k, new[k])
    energy = e_part[...]
    for w in (0, 1):
        h = field(get_a, weight, 1, even, w)
        new = heated(h, *trial_of(tb, w), beta)
        for k in range(3):
            put(out, 3 + 3 * w + k, new[k])
        energy = energy + dot3(new, h)
    mine = jnp.full(e_out.shape, -jnp.sum(energy), F32)
    if u == 1:
        lane = lax.broadcasted_iota(jnp.int32, e_out.shape, 1)
        other = jnp.broadcast_to(e_other[0:1, : e_out.shape[1]], e_out.shape)
        mine = jnp.where(lane == 0, other, mine)
    e_out[...] = mine


def exchanged(u, info, note):
    place = lax.axis_index("temp")
    upper = slot_of(u) == 1
    ours = jnp.max(info[1:2, :]) > 0
    theirs = jnp.max(note[1:2, :]) > 0.5
    inside = jnp.where(upper, place != lax.axis_size("temp") - 1, place != 0)
    return jnp.logical_and(jnp.where(upper, ours, theirs), inside)


def out_kernel(planes, half, *refs):
    info0, info1, i0, i1, o0, o1, ri0, ri1, ro0, ro1, out_h, taken, out, sems = refs
    core = core_index()
    columns = out.shape[-1]
    pushes = []
    for u, info, own, other in ((0, info0, (i0, o0), (ri0, ro0)), (1, info1, (i1, o1), (ri1, ro1))):
        note = ri0[pl.ds(EARLY * half, 8), :] if u == 0 else ri1[pl.ds(EARLY * half, 8), :]
        take = exchanged(u, info, note)
        taken[u : u + 1, :] = jnp.full((1, columns), take.astype(jnp.int32), jnp.int32)

        def write(early, late, parities):
            even = (lax.broadcasted_iota(jnp.int32, (half, columns), 1) & 1) == jnp.broadcast_to(
                parities, (half, columns)
            )
            for w in range(planes):
                z = w + core * (planes - 1 - 2 * w)
                m = at_plane(even, w)
                for k in range(3):
                    a = tile(late, k, half) if w == 0 else tile(early, 3 * (w - 1) + k, half)
                    b = tile(late, 3 + 3 * w + k, half) if w < 2 else tile(early, 3 + 3 * w + k, half)
                    out[u, k, z, pl.ds(0, half, stride=2), :] = jnp.where(m, a, b)
                    out[u, k, z, pl.ds(1, half, stride=2), :] = jnp.where(m, b, a)

        @pl.when(take)
        def _():
            write(*other, note[0:1, :].astype(jnp.int32))

        @pl.when(jnp.logical_not(take))
        def _():
            write(*own, info[0:1, :])

        push = pltpu.make_async_copy(out.at[u], out_h.at[slot_of(u)], sems.at[u])
        push.start()
        pushes.append(push)
    for push in pushes:
        push.wait()


def partner_of(u):
    place, temps = lax.axis_index("temp"), lax.axis_size("temp")
    odd = lax.rem(place, 2)
    step = 1 - 2 * odd if u == 0 else 2 * odd - 1
    return lax.rem(place + step + temps, temps)


def energy_kernel(count, sites, taken, parts, energies_h, energies, sem):
    def total(place):
        rows = parts[pl.ds(pl.multiple_of(place * count, count), count), :]
        return jnp.sum(rows, axis=0, keepdims=True) / sites

    own = total(lax.axis_index("temp"))
    final = [
        jnp.where(taken[u : u + 1, u : u + 1] > 0, total(partner_of(u))[:, u : u + 1], own[:, u : u + 1])
        for u in range(2)
    ]
    lane = lax.broadcasted_iota(jnp.int32, energies.shape, 1)
    energies[...] = jnp.where(
        lane == slot_of(0),
        jnp.broadcast_to(final[0], energies.shape),
        jnp.broadcast_to(final[1], energies.shape),
    )
    copy = pltpu.make_async_copy(energies, energies_h, sem)
    copy.start()
    copy.wait()


def step(
    spin_state, couplings, inverse_temps, colour_order, heat_level, heat_height, heat_angle, swap_bits
):
    replicas, _, planes, rows, columns = spin_state.shape
    half = rows // 2
    count = lax.axis_size("gz")
    temps = lax.axis_size("temp")
    assert replicas == 2 and planes == 4 and rows % 2 == 0 and columns % 2 == 0
    assert count % 2 == 0 and temps % 2 == 0
    in_chip = [(i, i ^ 1) for i in range(count)]
    cross = [(i, (i + (1 if i % 2 else -1)) % count) for i in range(count)]
    partners = (
        [(i, i ^ 1) for i in range(temps)],
        [(i, (i + (1 if i % 2 else -1)) % temps) for i in range(temps)],
    )

    def swap_in(value):
        return lax.ppermute(value, "gz", in_chip)

    def swap_cross(value):
        return lax.ppermute(value, "gz", cross)

    def away(value, u):
        return lax.ppermute(value, "temp", partners[u])

    spins = PIECES * half
    pair = vm(6 * half, columns)
    p0x, p1x, pi, am0, am1, info0, info1, beta0, beta1 = kernel_call(
        functools.partial(load_kernel, planes, half),
        [vm(spins + 4 * rows, columns), vm(spins, columns), vm(2 * spins + 4 * rows, columns)]
        + [pair] * 2
        + [vm(8, columns, dtype=jnp.int32)] * 2
        + [vm(8, columns)] * 2,
        [HBM] * 5,
        scratch=[
            pltpu.SMEM((replicas,), jnp.int32),
            pltpu.SMEM((replicas,), jnp.int32),
            pltpu.SMEM((replicas,), F32),
            vm(planes, replicas, 3, rows, columns),
            pltpu.SemaphoreType.DMA((3 + planes,)),
            pltpu.SemaphoreType.DMA((2, 4)),
        ],
    )(*(in_hbm(v) for v in (swap_bits, colour_order, inverse_temps, spin_state, couplings)))
    info, beta = [info0, info1], [beta0, beta1]
    sx, si, a_in, a_x = [p0x, p1x], [pi, pi], [am0, am1], [[], []]
    rx = [swap_cross(sx[u]) for u in range(2)]
    ri = swap_in(pi)

    ta0, tb0, ta1, tb1, dx, di = kernel_call(
        functools.partial(trial_kernel, planes, half),
        [vm(planes, 4, half, columns)] * 4 + [pair] * 2,
        [SM, SM, VM, VM, VM],
    )(swap_bits, colour_order, heat_level, heat_height, heat_angle)
    trial_a, trial_b = [ta0, ta1], [tb0, tb1]
    rdx, rdi = swap_cross(dx), swap_in(di)

    w_in = kernel_call(
        functools.partial(weight_kernel, planes, half, True),
        [vm(2, planes, 6, half, columns)] * 2,
        [VM] * 4,
    )(couplings, ri, info0, info1)
    w_x = kernel_call(
        functools.partial(weight_kernel, planes, half, False),
        [vm(2, 2, 6, half, columns)] * 2,
        [VM] * 4,
    )(couplings, rx[0], info0, info1)

    assert OR_SWEEPS == 2
    for sweep in range(OR_SWEEPS):
        first = sweep == 0
        new_in, bi = [None] * 2, [None] * 2
        for u in range(2):
            new_in[u], bi[u] = kernel_call(
                functools.partial(relax_early, planes, half, first, u),
                [vm(3 * planes * half, columns), vm(6 * (1 + u) * half, columns)],
                [VM] * (6 + u),
            )(info[u], w_in[u], sx[u], si[u], ri, a_in[u], *bi[:u])
        for u in range(2):
            *a_x[u], sx[u] = kernel_call(
                functools.partial(relax_late, planes, half, first),
                [pair] * (1 + first),
                [VM] * (6 if first else 7),
                scratch=[] if first else [pair],
            )(info[u], w_in[u], w_x[u], sx[u], rx[u], new_in[u], *a_x[u])
            si[u], a_in[u] = bi[u], new_in[u]
            rx[u] = swap_cross(sx[u])
        ri = swap_in(bi[1])

    inner, outer, part, r_inner, r_outer = ([None] * 2 for _ in range(5))
    for u in range(2):
        inner[u], part[u] = kernel_call(
            functools.partial(heat_early, planes, half, u),
            [vm(EARLY * half + 8, columns), vm(half, columns)],
            [VM] * 9,
            scratch=[vm(3, half, columns)],
        )(info[u], beta[u], w_in[u], sx[u], si[u], ri, trial_a[u], trial_b[u], rdi)
        r_inner[u] = away(inner[u], u)
    energy = []
    for u in range(2):
        outer[u], *energy = kernel_call(
            functools.partial(heat_late, planes, half, u),
            [vm(LATE * half, columns), vm(temps * count, 2) if u else vm(8, columns)],
            [VM] * (11 + u),
            scratch=[vm(3, half, columns)],
        )(
            info[u], beta[u], w_in[u], w_x[u], sx[u], rx[u],
            trial_a[u], trial_b[u], rdx, inner[u], part[u], *energy,
        )
        r_outer[u] = away(outer[u], u)

    parts = lax.all_to_all(energy[0], ("temp", "gz"), split_axis=0, concat_axis=0, tiled=True)

    spin_final, taken = kernel_call(
        functools.partial(out_kernel, planes, half),
        [jax.ShapeDtypeStruct(spin_state.shape, F32), vm(8, columns, dtype=jnp.int32)],
        [VM] * 10,
        out_specs=[HBM, VM],
        scratch=[vm(*spin_state.shape), pltpu.SemaphoreType.DMA((2,))],
    )(info0, info1, *inner, *outer, *r_inner, *r_outer)
    (energies,) = kernel_call(
        functools.partial(energy_kernel, count, float(columns * rows * planes * count)),
        [jax.ShapeDtypeStruct((1, 2), F32)],
        [VM] * 2,
        out_specs=[HBM],
        scratch=[vm(1, 2), pltpu.SemaphoreType.DMA(())],
    )(taken, parts)
    return spin_final, energies.reshape(-1)


def solution(mesh):
    return jax.shard_map(
        step,
        mesh=mesh,
        in_specs=(
            P(("group", "temp"), None, "gz", None, None),
            P(None, ("group", "gz"), None, None),
            P(("group", "temp")),
            P(("group", "temp")),
            P(("group", "temp"), "gz", None, None),
            P(("group", "temp"), "gz", None, None),
            P(("group", "temp"), "gz", None, None),
            P(("group", "temp")),
        ),
        out_specs=(P(("group", "temp"), None, "gz", None, None), P(("group", "temp"))),
        check_vma=False,
    )
```

```python
import functools

import jax
import jax.numpy as jnp
from jax import lax
from jax.experimental import pallas as pl
from jax.experimental.pallas import tpu as pltpu
from jax.sharding import PartitionSpec as P


F32 = jnp.float32
OR_SWEEPS = 2


VM = pl.BlockSpec(memory_space=pltpu.VMEM)
SM = pl.BlockSpec(memory_space=pltpu.SMEM)
ANY = pl.BlockSpec(memory_space=pl.ANY)
HBM = pl.BlockSpec(memory_space=pltpu.HBM)
PIECES = 9
EARLY = 15
LATE = 9


def vm(*shape, dtype=F32):
    return pltpu.VMEM(shape, dtype)


def kernel_call(body, outs, in_specs, out_specs=None, scratch=(), mib=24):
    return pl.pallas_call(
        body,
        out_shape=outs,
        in_specs=in_specs,
        out_specs=out_specs if out_specs is not None else [VM] * len(outs),
        scratch_shapes=list(scratch),
        compiler_params=pltpu.CompilerParams(vmem_limit_bytes=mib * 1024 * 1024),
    )


def in_hbm(value):
    return pltpu.with_memory_space_constraint(value, pltpu.HBM)


def core_index():
    return lax.rem(lax.axis_index("gz"), 2)


def slot_of(u):
    odd = lax.rem(lax.axis_index("temp"), 2)
    return 1 - odd if u == 0 else odd


def slot_replica(swap, u):
    return slot_of(u) ^ (swap[0] != 0).astype(jnp.int32)


def lane_even(rows, columns, offset):
    lane = lax.broadcasted_iota(jnp.int32, (rows, columns), 1)
    return ((lane + offset) & 1) == 0


def tile(ref, i, half):
    return ref[pl.ds(i * half, half), :]


def put(ref, i, value):
    half = value.shape[0]
    ref[pl.ds(i * half, half), :] = value


def folded(ref, index, half):
    return tuple(ref[(*index, pl.ds(s, half, stride=2), slice(None))] for s in (0, 1))


def folded_rows(ref, base, half):
    return tuple(ref[pl.ds(base + s, half, stride=2), :] for s in (0, 1))


def parity(info, half):
    columns = info.shape[-1]
    lane = lax.broadcasted_iota(jnp.int32, (half, columns), 1)
    return (lane & 1) == jnp.broadcast_to(info[0:1, :], (half, columns))


def at_plane(even, w):
    return even if w % 2 == 0 else jnp.logical_not(even)


def bond_copies(planes, coup, target, base, rows, side_in, sems):
    core = core_index()
    top = planes - 1
    at_top = 1 - core if side_in else core
    z = at_top * top
    return [
        pltpu.make_async_copy(coup.at[d, p], target.at[pl.ds(base + i * rows, rows), :], sems.at[i])
        for i, (d, p) in enumerate(((0, z), (1, z), (2, at_top * (top - 1)), (2, z)))
    ]


def load_kernel(planes, half, in_chip, *refs):
    swap_h, colour_h, beta_h, spin_h, coup_h = refs[:5]
    if in_chip:
        pi, am0, am1 = refs[5:8]
    else:
        p0x, p1x, am0, am1, info0, info1, beta0, beta1 = refs[5:13]
    swap, colour, betas, spin, sems, bond_sems = refs[-6:]
    core = core_index()
    columns = spin.shape[-1]
    rows = 2 * half
    top = planes - 1
    sides = (planes - 1, planes - 2) if in_chip else (0, 1)
    scalars = [
        pltpu.make_async_copy(swap_h, swap, sems.at[0]),
        pltpu.make_async_copy(colour_h, colour, sems.at[1]),
        pltpu.make_async_copy(beta_h, betas, sems.at[2]),
    ]
    spins = [
        pltpu.make_async_copy(spin_h.at[:, :, w + core * (top - 2 * w)], spin.at[i], sems.at[3 + i])
        for i, w in enumerate(sides)
    ]
    payload, base = (pi, 2 * PIECES * half) if in_chip else (p0x, PIECES * half)
    bonds = bond_copies(planes, coup_h, payload, base, rows, in_chip, bond_sems)
    for copy in scalars + spins + bonds:
        copy.start()
    for copy in scalars:
        copy.wait()
    reps, masks = [], []
    for u in range(2):
        rep = slot_replica(swap, u)
        c = colour[rep] ^ core
        if not in_chip:
            info, beta = ((info0, beta0), (info1, beta1))[u]
            info[0:1, :] = jnp.full((1, columns), c, jnp.int32)
            info[1:2, :] = jnp.full((1, columns), (swap[1] != 0).astype(jnp.int32), jnp.int32)
            beta[...] = jnp.full(beta.shape, betas[rep], F32)
        reps.append(rep)
        masks.append(lane_even(half, columns, c))
    for i, w in enumerate(sides):
        spins[i].wait()
        for u, am in ((0, am0), (1, am1)):
            side, base = (pi, PIECES * u) if in_chip else ((p0x, p1x)[u], 0)
            m = at_plane(masks[u], w)
            for k in range(3):
                even, odd = folded(spin, (i, reps[u], k), half)
                a = jnp.where(m, even, odd)
                b = jnp.where(m, odd, even)
                put(side, base + 3 * i + k, b)
                if i == 0:
                    put(side, base + 6 + k, a)
                else:
                    put(am, k, a)
    for copy in bonds:
        copy.wait()


def weight_kernel(planes, half, in_chip, *refs):
    coup, sent_ref, info0, info1, weights0, weights1 = refs
    core = core_index()
    top = planes - 1
    rows = 2 * half
    first = core == 0

    def sent(i):
        return folded_rows(sent_ref, (2 if in_chip else 1) * PIECES * half + i * rows, half)

    def zbond(m):
        if m in (-1, planes + 1):
            return sent(2)
        if m in (0, planes):
            ours, theirs = folded(coup, (2, top), half), sent(3)
            mine = first if m == planes else jnp.logical_not(first)
            return tuple(jnp.where(mine, o, t) for o, t in zip(ours, theirs))
        return folded(coup, (2, (m - 1) + core * (top - 2 * m + 1)), half)

    span = range(1, planes + 1) if in_chip else range(-1, 1)
    below = zbond(span[0])
    for i, w in enumerate(span):
        above = zbond(w + 1)
        if w in (-1, planes):
            jx, jy = sent(0), sent(1)
        else:
            z = w + core * (top - 2 * w)
            jx, jy = folded(coup, (0, z), half), folded(coup, (1, z), half)
        up_odd = pltpu.roll(jy[1], 1, 0)
        for info, weights in ((info0, weights0), (info1, weights1)):
            even = parity(info, half)
            for a in (0, 1):
                if a == 1 and w in (-1, planes):
                    continue
                m = at_plane(even, w + a)
                weights[a, i, 0] = jnp.where(m, jx[0], jx[1])
                weights[a, i, 1] = pltpu.roll(jnp.where(m, jx[1], jx[0]), 1, 1)
                weights[a, i, 2] = jy[0]
                weights[a, i, 3] = jnp.where(m, up_odd, jy[1])
                weights[a, i, 4] = jnp.where(m, above[0], above[1])
                weights[a, i, 5] = jnp.where(m, below[0], below[1])
        below = above


def field(get, weight, a, even, w):
    total = []
    m = at_plane(even, w + a)
    for k in range(3):
        o = get(w, k)
        half, columns = o.shape
        side = jnp.where(m, pltpu.roll(o, 1, 0), pltpu.roll(o, half - 1, 0))
        h = weight(a, w, 0) * pltpu.roll(o, columns - 1, 1)
        h = h + weight(a, w, 1) * pltpu.roll(o, 1, 1)
        h = h + weight(a, w, 2) * o
        h = h + weight(a, w, 3) * side
        h = h + weight(a, w, 4) * get(w + 1, k)
        h = h + weight(a, w, 5) * get(w - 1, k)
        total.append(h)
    return total


def weight_of(w_in, w_x):
    return lambda a, w, i: w_in[a, w - 1, i] if w > 0 else w_x[a, w + 1, i]


def dot3(a, b):
    return a[0] * b[0] + a[1] * b[1] + a[2] * b[2]


def reflect(s, h):
    f = 2.0 * dot3(s, h) / jnp.maximum(dot3(h, h), 0.01)
    return [f * h[k] - s[k] for k in range(3)]


def second_planes(planes, half, sx, si, rx, ri, own=0, sent=0):
    def get(w, k):
        if w < 0:
            return tile(rx, 3 * (-1 - w) + k, half)
        if w < 2:
            return tile(sx, 3 * w + k, half)
        if w < planes:
            return tile(si, own + 3 * (planes - 1 - w) + k, half)
        return tile(ri, sent + 3 * (w - planes) + k, half)

    return get


def relax_early(planes, half, first, u, *refs):
    info, w_in, sx, si, ri, *a_old = refs[: 7 if first else 6]
    a_new, bi = refs[-2:]
    offset = (PIECES if first else 6) * u
    even = parity(info, half)
    weight = weight_of(w_in, None)
    get_b = second_planes(planes, half, sx, si, None, ri, offset, offset)
    if u == 1:
        bi[pl.ds(0, 6 * half), :] = refs[-3][...]

    def get_a(w, k):
        if not first:
            return tile(a_old[0], 3 * (w - 1) + k, half)
        if w == planes - 1:
            return tile(si, offset + 6 + k, half)
        if w == planes:
            return tile(ri, offset + 6 + k, half)
        return tile(a_old[w - 1], k, half)

    for w in range(1, planes + 1):
        h = field(get_b, weight, 0, even, w)
        new = reflect([get_a(w, k) for k in range(3)], h)
        for k in range(3):
            put(a_new, 3 * (w - 1) + k, new[k])
    for w in range(2, planes):
        h = field(lambda v, k: tile(a_new, 3 * (v - 1) + k, half), weight, 1, even, w)
        new = reflect([get_b(w, k) for k in range(3)], h)
        for k in range(3):
            put(bi, 6 * u + 3 * (planes - 1 - w) + k, new[k])


def relax_late(planes, half, first, *refs):
    info, w_in, w_x, sx, rx, a_in = refs[:6]
    a_old, a_new, bx = (None, *refs[6:]) if first else (refs[6], refs[8], refs[7])
    even = parity(info, half)
    weight = weight_of(w_in, w_x)
    get_b = second_planes(planes, half, sx, None, rx, None)

    def get_a(w, k):
        if not first:
            return tile(a_old, 3 * (w + 1) + k, half)
        return tile(rx if w < 0 else sx, 6 + k, half)

    for w in (-1, 0):
        h = field(get_b, weight, 0, even, w)
        new = reflect([get_a(w, k) for k in range(3)], h)
        for k in range(3):
            put(a_new, 3 * (w + 1) + k, new[k])

    def get_new(w, k):
        return tile(a_new, 3 * (w + 1) + k, half) if w < 1 else tile(a_in, 3 * (w - 1) + k, half)

    for w in (0, 1):
        h = field(get_new, weight, 1, even, w)
        new = reflect([get_b(w, k) for k in range(3)], h)
        for k in range(3):
            put(bx, 3 * w + k, new[k])


SIN = (1.0, -1 / 6, 1 / 120, -1 / 5040, 1 / 362880, -1 / 39916800, 1 / 6227020800)
COS = (1.0, -1 / 2, 1 / 24, -1 / 720, 1 / 40320, -1 / 3628800, 1 / 479001600, -1 / 87178291200)


def series(coefficients, y):
    total = coefficients[-1]
    for value in coefficients[-2::-1]:
        total = total * y + value
    return total


def trial(height, angle):
    t = 0.5 * angle
    y = t * t
    s = t * series(SIN, y)
    c = series(COS, y)
    q = jnp.sqrt(jnp.maximum(1.0 - height * height, 0.0))
    return q * (1.0 - 2.0 * (s * s)), q * (2.0 * (s * c))


def trial_kernel(planes, half, swap, colour, level, height, angle, ta0, tb0, ta1, tb1, dx, di):
    core = core_index()
    columns = level.shape[-1]
    for u, ta, tb in ((0, ta0, tb0), (1, ta1, tb1)):
        rep = slot_replica(swap, u)
        c = colour[rep]
        for w in range(planes):
            z = w + core * (planes - 1 - 2 * w)
            m = lane_even(half, columns, z + c)
            a, b = [], []
            for ref in (level, height, angle):
                even, odd = folded(ref, (rep, z), half)
                a.append(jnp.where(m, even, odd))
                b.append(jnp.where(m, odd, even))
            if w == 0 or w == planes - 1:
                for i in range(3):
                    put(dx if w == 0 else di, 3 * u + i, a[i])
            for t, (lev, hei, ang) in ((ta, a), (tb, b)):
                ux, uy = trial(hei, ang)
                t[w, 0], t[w, 1], t[w, 2], t[w, 3] = ux, uy, hei, lev


def trial_of(t, w):
    return [t[w, k] for k in range(3)], t[w, 3]


def trial_sent(draws, u, half):
    level, height, angle = (tile(draws, 3 * u + i, half) for i in range(3))
    ux, uy = trial(height, angle)
    return [ux, uy, height], level


def heated(h, u, level, beta):
    m = jnp.maximum(dot3(h, h), 0.01)
    inverse = lax.rsqrt(m)
    e = [h[k] * inverse for k in range(3)]
    reach = beta * (m * inverse)
    c = 1.0 + jnp.log(1.0 + level * (jnp.exp(-2.0 * reach) - 1.0)) / reach
    along = dot3(u, e)
    t = [u[k] - along * e[k] for k in range(3)]
    f = jnp.sqrt(jnp.maximum(1.0 - c * c, 0.0)) * lax.rsqrt(jnp.maximum(dot3(t, t), 0.0001))
    return [c * e[k] + f * t[k] for k in range(3)]


def heat_early(planes, half, u, *refs):
    info, betas, w_in, sx, si, ri, ta, tb, rdi, out, e_part, halo = refs
    even = parity(info, half)
    columns = info.shape[-1]
    beta = jnp.broadcast_to(betas[0:1, :], (half, columns))
    weight = weight_of(w_in, None)
    get_b = second_planes(planes, half, sx, si, None, ri, 6 * u, 6 * u)

    def get_a(w, k):
        return halo[k] if w == planes else tile(out, 3 * (w - 1) + k, half)

    for w in range(1, planes + 1):
        h = field(get_b, weight, 0, even, w)
        draw = trial_of(ta, w) if w < planes else trial_sent(rdi, u, half)
        new = heated(h, *draw, beta)
        for k in range(3):
            if w == planes:
                halo[k] = new[k]
            else:
                put(out, 3 * (w - 1) + k, new[k])
    energy = None
    for w in range(2, planes):
        h = field(get_a, weight, 1, even, w)
        new = heated(h, *trial_of(tb, w), beta)
        for k in range(3):
            put(out, 9 + 3 * (w - 2) + k, new[k])
        term = dot3(new, h)
        energy = term if energy is None else energy + term
    e_part[...] = energy
    out[pl.ds(EARLY * half, 8), :] = info[...].astype(F32)


def heat_late(planes, half, u, *refs):
    info, betas, w_in, w_x, sx, rx, ta, tb, rdx, inner, e_part = refs[:11]
    if u == 0:
        out, e_out, halo = refs[11:]
    else:
        e_other, out, e_out, halo = refs[11:]
    even = parity(info, half)
    columns = info.shape[-1]
    beta = jnp.broadcast_to(betas[0:1, :], (half, columns))
    weight = weight_of(w_in, w_x)
    get_b = second_planes(planes, half, sx, None, rx, None)

    def get_a(w, k):
        if w < 0:
            return halo[k]
        return tile(out, k, half) if w == 0 else tile(inner, 3 * (w - 1) + k, half)

    for w in (-1, 0):
        h = field(get_b, weight, 0, even, w)
        draw = trial_of(ta, w) if w >= 0 else trial_sent(rdx, u, half)
        new = heated(h, *draw, beta)
        for k in range(3):
            if w < 0:
                halo[k] = new[k]
            else:
                put(out, k, new[k])
    energy = e_part[...]
    for w in (0, 1):
        h = field(get_a, weight, 1, even, w)
        new = heated(h, *trial_of(tb, w), beta)
        for k in range(3):
            put(out, 3 + 3 * w + k, new[k])
        energy = energy + dot3(new, h)
    mine = jnp.full(e_out.shape, -jnp.sum(energy), F32)
    if u == 1:
        lane = lax.broadcasted_iota(jnp.int32, e_out.shape, 1)
        other = jnp.broadcast_to(e_other[0:1, : e_out.shape[1]], e_out.shape)
        mine = jnp.where(lane == 0, other, mine)
    e_out[...] = mine


def total_kernel(sites, parts, total):
    total[...] = jnp.sum(parts[...], axis=0, keepdims=True) / sites


def exchanged(u, info, note):
    place = lax.axis_index("temp")
    upper = slot_of(u) == 1
    ours = jnp.max(info[1:2, :]) > 0
    theirs = jnp.max(note[1:2, :]) > 0.5
    inside = jnp.where(upper, place != lax.axis_size("temp") - 1, place != 0)
    return jnp.logical_and(jnp.where(upper, ours, theirs), inside)


def out_kernel(planes, half, *refs):
    info0, info1, i0, i1, o0, o1, ri0, ri1, ro0, ro1, out_h, taken, out, sems = refs
    core = core_index()
    columns = out.shape[-1]
    sources = []
    for u, info, own, other in ((0, info0, (i0, o0), (ri0, ro0)), (1, info1, (i1, o1), (ri1, ro1))):
        note = other[0][pl.ds(EARLY * half, 8), :]
        take = exchanged(u, info, note)
        taken[u : u + 1, :] = jnp.full((1, columns), take.astype(jnp.int32), jnp.int32)
        sources.append((take, (*other, note[0:1, :].astype(jnp.int32)), (*own, info[0:1, :])))
    pushes = []
    for u, (take, theirs, ours) in enumerate(sources):
        for w in range(planes):
            z = w + core * (planes - 1 - 2 * w)

            def write(early, late, parities):
                lane = lax.broadcasted_iota(jnp.int32, (half, columns), 1)
                m = at_plane((lane & 1) == jnp.broadcast_to(parities, (half, columns)), w)
                for k in range(3):
                    a = tile(late, k, half) if w == 0 else tile(early, 3 * (w - 1) + k, half)
                    b = tile(late, 3 + 3 * w + k, half) if w < 2 else tile(early, 3 + 3 * w + k, half)
                    out[u, w, k, pl.ds(0, half, stride=2), :] = jnp.where(m, a, b)
                    out[u, w, k, pl.ds(1, half, stride=2), :] = jnp.where(m, b, a)

            pl.when(take)(functools.partial(write, *theirs))
            pl.when(jnp.logical_not(take))(functools.partial(write, *ours))
            push = pltpu.make_async_copy(out.at[u, w], out_h.at[slot_of(u), :, z], sems.at[u, w])
            push.start()
            pushes.append(push)
    for push in pushes:
        push.wait()


def energy_kernel(taken, total, r0, r1, energies_h, energies, sem):
    final = [
        jnp.where(taken[u : u + 1, u : u + 1] > 0, r[:, u : u + 1], total[:, u : u + 1])
        for u, r in ((0, r0), (1, r1))
    ]
    lane = lax.broadcasted_iota(jnp.int32, energies.shape, 1)
    energies[...] = jnp.where(
        lane == slot_of(0),
        jnp.broadcast_to(final[0], energies.shape),
        jnp.broadcast_to(final[1], energies.shape),
    )
    copy = pltpu.make_async_copy(energies, energies_h, sem)
    copy.start()
    copy.wait()


def step(
    spin_state, couplings, inverse_temps, colour_order, heat_level, heat_height, heat_angle, swap_bits
):
    replicas, _, planes, rows, columns = spin_state.shape
    half = rows // 2
    count = lax.axis_size("gz")
    temps = lax.axis_size("temp")
    assert replicas == 2 and planes == 4 and rows % 2 == 0 and columns % 2 == 0
    assert count % 2 == 0 and temps % 2 == 0
    in_chip = [(i, i ^ 1) for i in range(count)]
    cross = [(i, (i + (1 if i % 2 else -1)) % count) for i in range(count)]
    partners = (
        [(i, i ^ 1) for i in range(temps)],
        [(i, (i + (1 if i % 2 else -1)) % temps) for i in range(temps)],
    )

    def swap_in(value):
        return lax.ppermute(value, "gz", in_chip)

    def swap_cross(value):
        return lax.ppermute(value, "gz", cross)

    def away(value, u):
        return lax.ppermute(value, "temp", partners[u])

    spins = PIECES * half
    pair = vm(6 * half, columns)
    raw = [in_hbm(v) for v in (swap_bits, colour_order, inverse_temps, spin_state, couplings)]
    plane = vm(3 * half, columns)
    scratch = [
        pltpu.SMEM((replicas,), jnp.int32),
        pltpu.SMEM((replicas,), jnp.int32),
        pltpu.SMEM((replicas,), F32),
        vm(2, replicas, 3, rows, columns),
        pltpu.SemaphoreType.DMA((5,)),
        pltpu.SemaphoreType.DMA((4,)),
    ]
    p0x, p1x, ax0, ax1, info0, info1, beta0, beta1 = kernel_call(
        functools.partial(load_kernel, planes, half, False),
        [vm(spins + 4 * rows, columns), vm(spins, columns), plane, plane]
        + [vm(8, columns, dtype=jnp.int32)] * 2
        + [vm(8, columns)] * 2,
        [HBM] * 5,
        scratch=scratch,
    )(*raw)
    pi, ai0, ai1 = kernel_call(
        functools.partial(load_kernel, planes, half, True),
        [vm(2 * spins + 4 * rows, columns), plane, plane],
        [HBM] * 5,
        scratch=scratch,
    )(*raw)
    info, beta = [info0, info1], [beta0, beta1]
    sx, si, a_in, a_x = [p0x, p1x], [pi, pi], [(ax0, ai0), (ax1, ai1)], [[], []]
    rx = [swap_cross(sx[u]) for u in range(2)]
    ri = swap_in(pi)

    ta0, tb0, ta1, tb1, dx, di = kernel_call(
        functools.partial(trial_kernel, planes, half),
        [vm(planes, 4, half, columns)] * 4 + [pair] * 2,
        [SM, SM, VM, VM, VM],
    )(swap_bits, colour_order, heat_level, heat_height, heat_angle)
    trial_a, trial_b = [ta0, ta1], [tb0, tb1]
    rdx, rdi = swap_cross(dx), swap_in(di)

    w_in = kernel_call(
        functools.partial(weight_kernel, planes, half, True),
        [vm(2, planes, 6, half, columns)] * 2,
        [VM] * 4,
    )(couplings, ri, info0, info1)
    w_x = kernel_call(
        functools.partial(weight_kernel, planes, half, False),
        [vm(2, 2, 6, half, columns)] * 2,
        [VM] * 4,
    )(couplings, rx[0], info0, info1)

    assert OR_SWEEPS == 2
    for sweep in range(OR_SWEEPS):
        first = sweep == 0
        new_in, bi = [None] * 2, [None] * 2
        for u in range(2):
            new_in[u], bi[u] = kernel_call(
                functools.partial(relax_early, planes, half, first, u),
                [vm(3 * planes * half, columns), vm(6 * (1 + u) * half, columns)],
                [VM] * (6 + first + u),
            )(info[u], w_in[u], sx[u], si[u], ri, *a_in[u], *bi[:u])
        for u in range(2):
            *a_x[u], sx[u] = kernel_call(
                functools.partial(relax_late, planes, half, first),
                [pair] * (1 + first),
                [VM] * (6 if first else 7),
                scratch=[] if first else [pair],
            )(info[u], w_in[u], w_x[u], sx[u], rx[u], new_in[u], *a_x[u])
            si[u], a_in[u] = bi[u], [new_in[u]]
            rx[u] = swap_cross(sx[u])
        ri = swap_in(bi[1])

    inner, outer, part, r_inner, r_outer = ([None] * 2 for _ in range(5))
    for u in range(2):
        inner[u], part[u] = kernel_call(
            functools.partial(heat_early, planes, half, u),
            [vm(EARLY * half + 8, columns), vm(half, columns)],
            [VM] * 9,
            scratch=[vm(3, half, columns)],
        )(info[u], beta[u], w_in[u], sx[u], si[u], ri, trial_a[u], trial_b[u], rdi)
        r_inner[u] = away(inner[u], u)
    energy = []
    for u in range(2):
        outer[u], *energy = kernel_call(
            functools.partial(heat_late, planes, half, u),
            [vm(LATE * half, columns), vm(count, 2) if u else vm(8, columns)],
            [VM] * (11 + u),
            scratch=[vm(3, half, columns)],
        )(
            info[u], beta[u], w_in[u], w_x[u], sx[u], rx[u],
            trial_a[u], trial_b[u], rdx, inner[u], part[u], *energy,
        )
        r_outer[u] = away(outer[u], u)

    parts = lax.all_to_all(energy[0], "gz", split_axis=0, concat_axis=0, tiled=True)
    (total,) = kernel_call(
        functools.partial(total_kernel, float(columns * rows * planes * count)), [vm(1, 2)], [VM]
    )(parts)
    r_total = [away(total, u) for u in range(2)]

    spin_final, taken = kernel_call(
        functools.partial(out_kernel, planes, half),
        [jax.ShapeDtypeStruct(spin_state.shape, F32), vm(8, columns, dtype=jnp.int32)],
        [VM] * 10,
        out_specs=[HBM, VM],
        scratch=[vm(2, planes, 3, rows, columns), pltpu.SemaphoreType.DMA((2, planes))],
    )(info0, info1, *inner, *outer, *r_inner, *r_outer)
    (energies,) = kernel_call(
        energy_kernel,
        [jax.ShapeDtypeStruct((1, 2), F32)],
        [VM] * 4,
        out_specs=[HBM],
        scratch=[vm(1, 2), pltpu.SemaphoreType.DMA(())],
    )(taken, total, *r_total)
    return spin_final, energies.reshape(-1)


def solution(mesh):
    return jax.shard_map(
        step,
        mesh=mesh,
        in_specs=(
            P(("group", "temp"), None, "gz", None, None),
            P(None, ("group", "gz"), None, None),
            P(("group", "temp")),
            P(("group", "temp")),
            P(("group", "temp"), "gz", None, None),
            P(("group", "temp"), "gz", None, None),
            P(("group", "temp"), "gz", None, None),
            P(("group", "temp")),
        ),
        out_specs=(P(("group", "temp"), None, "gz", None, None), P(("group", "temp"))),
        check_vma=False,
    )
```

```python
import functools

import jax
import jax.numpy as jnp
from jax import lax
from jax.experimental import pallas as pl
from jax.experimental.pallas import tpu as pltpu
from jax.sharding import PartitionSpec as P


F32 = jnp.float32
OR_SWEEPS = 2


VM = pl.BlockSpec(memory_space=pltpu.VMEM)
SM = pl.BlockSpec(memory_space=pltpu.SMEM)
ANY = pl.BlockSpec(memory_space=pl.ANY)
HBM = pl.BlockSpec(memory_space=pltpu.HBM)
PIECES = 9
EARLY = 15
LATE = 9


def vm(*shape, dtype=F32):
    return pltpu.VMEM(shape, dtype)


def kernel_call(body, outs, in_specs, out_specs=None, scratch=(), mib=24):
    return pl.pallas_call(
        body,
        out_shape=outs,
        in_specs=in_specs,
        out_specs=out_specs if out_specs is not None else [VM] * len(outs),
        scratch_shapes=list(scratch),
        compiler_params=pltpu.CompilerParams(vmem_limit_bytes=mib * 1024 * 1024),
    )


def in_hbm(value):
    return pltpu.with_memory_space_constraint(value, pltpu.HBM)


def core_index():
    return lax.rem(lax.axis_index("gz"), 2)


def slot_of(u):
    odd = lax.rem(lax.axis_index("temp"), 2)
    return 1 - odd if u == 0 else odd


def slot_replica(swap, u):
    return slot_of(u) ^ (swap[0] != 0).astype(jnp.int32)


def lane_even(rows, columns, offset):
    lane = lax.broadcasted_iota(jnp.int32, (rows, columns), 1)
    return ((lane + offset) & 1) == 0


def tile(ref, i, half):
    return ref[pl.ds(i * half, half), :]


def put(ref, i, value):
    half = value.shape[0]
    ref[pl.ds(i * half, half), :] = value


def folded(ref, index, half):
    return tuple(ref[(*index, pl.ds(s, half, stride=2), slice(None))] for s in (0, 1))


def folded_rows(ref, base, half):
    return tuple(ref[pl.ds(base + s, half, stride=2), :] for s in (0, 1))


def parity(info, half):
    columns = info.shape[-1]
    lane = lax.broadcasted_iota(jnp.int32, (half, columns), 1)
    return (lane & 1) == jnp.broadcast_to(info[0:1, :], (half, columns))


def at_plane(even, w):
    return even if w % 2 == 0 else jnp.logical_not(even)


def bond_copies(planes, coup, target, base, rows, side_in, sems):
    core = core_index()
    top = planes - 1
    at_top = 1 - core if side_in else core
    z = at_top * top
    return [
        pltpu.make_async_copy(coup.at[d, p], target.at[pl.ds(base + i * rows, rows), :], sems.at[i])
        for i, (d, p) in enumerate(((0, z), (1, z), (2, at_top * (top - 1)), (2, z)))
    ]


def load_kernel(planes, half, *refs):
    (swap_h, colour_h, beta_h, spin_h, coup_h) = refs[:5]
    p0x, p1x, pi, am0, am1, info0, info1, beta0, beta1 = refs[5:14]
    swap, colour, betas, spin, sems, bond_sems = refs[14:]
    core = core_index()
    columns = spin.shape[-1]
    rows = 2 * half
    top = planes - 1
    scalars = [
        pltpu.make_async_copy(swap_h, swap, sems.at[0]),
        pltpu.make_async_copy(colour_h, colour, sems.at[1]),
        pltpu.make_async_copy(beta_h, betas, sems.at[2]),
    ]
    spins = [
        pltpu.make_async_copy(spin_h.at[:, :, w + core * (top - 2 * w)], spin.at[w], sems.at[3 + w])
        for w in range(planes)
    ]
    bonds = bond_copies(planes, coup_h, p0x, PIECES * half, rows, False, bond_sems.at[0])
    bonds += bond_copies(planes, coup_h, pi, 2 * PIECES * half, rows, True, bond_sems.at[1])
    for copy in scalars + spins + bonds:
        copy.start()
    for copy in scalars:
        copy.wait()
    reps, masks = [], []
    for u, info, beta in ((0, info0, beta0), (1, info1, beta1)):
        rep = slot_replica(swap, u)
        c = colour[rep] ^ core
        info[0:1, :] = jnp.full((1, columns), c, jnp.int32)
        info[1:2, :] = jnp.full((1, columns), (swap[1] != 0).astype(jnp.int32), jnp.int32)
        beta[...] = jnp.full(beta.shape, betas[rep], F32)
        reps.append(rep)
        masks.append(lane_even(half, columns, c))
    for w in range(planes):
        spins[w].wait()
        for u, sx, am in ((0, p0x, am0), (1, p1x, am1)):
            base = PIECES * u
            m = at_plane(masks[u], w)
            for k in range(3):
                even, odd = folded(spin, (w, reps[u], k), half)
                a = jnp.where(m, even, odd)
                b = jnp.where(m, odd, even)
                if w == 0:
                    put(sx, k, b)
                    put(sx, 6 + k, a)
                elif w == 1:
                    put(sx, 3 + k, b)
                    put(am, k, a)
                elif w == planes - 2:
                    put(pi, base + 3 + k, b)
                    put(am, 3 + k, a)
                else:
                    put(pi, base + k, b)
                    put(pi, base + 6 + k, a)
    for copy in bonds:
        copy.wait()


def weight_kernel(planes, half, in_chip, *refs):
    coup, sent_ref, info0, info1, weights0, weights1 = refs
    core = core_index()
    top = planes - 1
    rows = 2 * half
    first = core == 0

    def sent(i):
        return folded_rows(sent_ref, (2 if in_chip else 1) * PIECES * half + i * rows, half)

    def zbond(m):
        if m in (-1, planes + 1):
            return sent(2)
        if m in (0, planes):
            ours, theirs = folded(coup, (2, top), half), sent(3)
            mine = first if m == planes else jnp.logical_not(first)
            return tuple(jnp.where(mine, o, t) for o, t in zip(ours, theirs))
        return folded(coup, (2, (m - 1) + core * (top - 2 * m + 1)), half)

    span = range(1, planes + 1) if in_chip else range(-1, 1)
    below = zbond(span[0])
    for i, w in enumerate(span):
        above = zbond(w + 1)
        if w in (-1, planes):
            jx, jy = sent(0), sent(1)
        else:
            z = w + core * (top - 2 * w)
            jx, jy = folded(coup, (0, z), half), folded(coup, (1, z), half)
        up_odd = pltpu.roll(jy[1], 1, 0)
        for info, weights in ((info0, weights0), (info1, weights1)):
            even = parity(info, half)
            for a in (0, 1):
                if a == 1 and w in (-1, planes):
                    continue
                m = at_plane(even, w + a)
                weights[a, i, 0] = jnp.where(m, jx[0], jx[1])
                weights[a, i, 1] = pltpu.roll(jnp.where(m, jx[1], jx[0]), 1, 1)
                weights[a, i, 2] = jy[0]
                weights[a, i, 3] = jnp.where(m, up_odd, jy[1])
                weights[a, i, 4] = jnp.where(m, above[0], above[1])
                weights[a, i, 5] = jnp.where(m, below[0], below[1])
        below = above


def field(get, weight, a, even, w):
    total = []
    m = at_plane(even, w + a)
    for k in range(3):
        o = get(w, k)
        half, columns = o.shape
        side = jnp.where(m, pltpu.roll(o, 1, 0), pltpu.roll(o, half - 1, 0))
        h = weight(a, w, 0) * pltpu.roll(o, columns - 1, 1)
        h = h + weight(a, w, 1) * pltpu.roll(o, 1, 1)
        h = h + weight(a, w, 2) * o
        h = h + weight(a, w, 3) * side
        h = h + weight(a, w, 4) * get(w + 1, k)
        h = h + weight(a, w, 5) * get(w - 1, k)
        total.append(h)
    return total


def weight_of(w_in, w_x):
    return lambda a, w, i: w_in[a, w - 1, i] if w > 0 else w_x[a, w + 1, i]


def dot3(a, b):
    return a[0] * b[0] + a[1] * b[1] + a[2] * b[2]


def reflect(s, h):
    f = 2.0 * dot3(s, h) / jnp.maximum(dot3(h, h), 0.01)
    return [f * h[k] - s[k] for k in range(3)]


def second_planes(planes, half, sx, si, rx, ri, own=0, sent=0):
    def get(w, k):
        if w < 0:
            return tile(rx, 3 * (-1 - w) + k, half)
        if w < 2:
            return tile(sx, 3 * w + k, half)
        if w < planes:
            return tile(si, own + 3 * (planes - 1 - w) + k, half)
        return tile(ri, sent + 3 * (w - planes) + k, half)

    return get


def relax_early(planes, half, first, u, *refs):
    info, w_in, sx, si, ri, a_old = refs[:6]
    a_new, bi = refs[-2:]
    offset = (PIECES if first else 6) * u
    even = parity(info, half)
    weight = weight_of(w_in, None)
    get_b = second_planes(planes, half, sx, si, None, ri, offset, offset)
    if u == 1:
        bi[pl.ds(0, 6 * half), :] = refs[6][...]

    def get_a(w, k):
        if not first:
            return tile(a_old, 3 * (w - 1) + k, half)
        if w == planes - 1:
            return tile(si, offset + 6 + k, half)
        if w == planes:
            return tile(ri, offset + 6 + k, half)
        return tile(a_old, 3 * (w - 1) + k, half)

    for w in range(1, planes + 1):
        h = field(get_b, weight, 0, even, w)
        new = reflect([get_a(w, k) for k in range(3)], h)
        for k in range(3):
            put(a_new, 3 * (w - 1) + k, new[k])
    for w in range(2, planes):
        h = field(lambda v, k: tile(a_new, 3 * (v - 1) + k, half), weight, 1, even, w)
        new = reflect([get_b(w, k) for k in range(3)], h)
        for k in range(3):
            put(bi, 6 * u + 3 * (planes - 1 - w) + k, new[k])


def relax_late(planes, half, first, *refs):
    info, w_in, w_x, sx, rx, a_in = refs[:6]
    a_old, a_new, bx = (None, *refs[6:]) if first else (refs[6], refs[8], refs[7])
    even = parity(info, half)
    weight = weight_of(w_in, w_x)
    get_b = second_planes(planes, half, sx, None, rx, None)

    def get_a(w, k):
        if not first:
            return tile(a_old, 3 * (w + 1) + k, half)
        return tile(rx if w < 0 else sx, 6 + k, half)

    for w in (-1, 0):
        h = field(get_b, weight, 0, even, w)
        new = reflect([get_a(w, k) for k in range(3)], h)
        for k in range(3):
            put(a_new, 3 * (w + 1) + k, new[k])

    def get_new(w, k):
        return tile(a_new, 3 * (w + 1) + k, half) if w < 1 else tile(a_in, 3 * (w - 1) + k, half)

    for w in (0, 1):
        h = field(get_new, weight, 1, even, w)
        new = reflect([get_b(w, k) for k in range(3)], h)
        for k in range(3):
            put(bx, 3 * w + k, new[k])


SIN = (1.0, -1 / 6, 1 / 120, -1 / 5040, 1 / 362880, -1 / 39916800, 1 / 6227020800)
COS = (1.0, -1 / 2, 1 / 24, -1 / 720, 1 / 40320, -1 / 3628800, 1 / 479001600, -1 / 87178291200)


def series(coefficients, y):
    total = coefficients[-1]
    for value in coefficients[-2::-1]:
        total = total * y + value
    return total


def trial(height, angle):
    t = 0.5 * angle
    y = t * t
    s = t * series(SIN, y)
    c = series(COS, y)
    q = jnp.sqrt(jnp.maximum(1.0 - height * height, 0.0))
    return q * (1.0 - 2.0 * (s * s)), q * (2.0 * (s * c))


def trial_kernel(planes, half, swap, colour, level, height, angle, ta0, tb0, ta1, tb1, dx, di):
    core = core_index()
    columns = level.shape[-1]
    for u, ta, tb in ((0, ta0, tb0), (1, ta1, tb1)):
        rep = slot_replica(swap, u)
        c = colour[rep]
        for w in range(planes):
            z = w + core * (planes - 1 - 2 * w)
            m = lane_even(half, columns, z + c)
            a, b = [], []
            for ref in (level, height, angle):
                even, odd = folded(ref, (rep, z), half)
                a.append(jnp.where(m, even, odd))
                b.append(jnp.where(m, odd, even))
            if w == 0 or w == planes - 1:
                for i in range(3):
                    put(dx if w == 0 else di, 3 * u + i, a[i])
            for t, (lev, hei, ang) in ((ta, a), (tb, b)):
                ux, uy = trial(hei, ang)
                t[w, 0], t[w, 1], t[w, 2], t[w, 3] = ux, uy, hei, lev


def trial_of(t, w):
    return [t[w, k] for k in range(3)], t[w, 3]


def trial_sent(draws, u, half):
    level, height, angle = (tile(draws, 3 * u + i, half) for i in range(3))
    ux, uy = trial(height, angle)
    return [ux, uy, height], level


def heated(h, u, level, beta):
    m = jnp.maximum(dot3(h, h), 0.01)
    inverse = lax.rsqrt(m)
    e = [h[k] * inverse for k in range(3)]
    reach = beta * (m * inverse)
    c = 1.0 + jnp.log(1.0 + level * (jnp.exp(-2.0 * reach) - 1.0)) / reach
    along = dot3(u, e)
    t = [u[k] - along * e[k] for k in range(3)]
    f = jnp.sqrt(jnp.maximum(1.0 - c * c, 0.0)) * lax.rsqrt(jnp.maximum(dot3(t, t), 0.0001))
    return [c * e[k] + f * t[k] for k in range(3)]


def heat_early(planes, half, u, *refs):
    info, betas, w_in, sx, si, ri, ta, tb, rdi, out, e_part, halo = refs
    even = parity(info, half)
    columns = info.shape[-1]
    beta = jnp.broadcast_to(betas[0:1, :], (half, columns))
    weight = weight_of(w_in, None)
    get_b = second_planes(planes, half, sx, si, None, ri, 6 * u, 6 * u)

    def get_a(w, k):
        return halo[k] if w == planes else tile(out, 3 * (w - 1) + k, half)

    for w in range(1, planes + 1):
        h = field(get_b, weight, 0, even, w)
        draw = trial_of(ta, w) if w < planes else trial_sent(rdi, u, half)
        new = heated(h, *draw, beta)
        for k in range(3):
            if w == planes:
                halo[k] = new[k]
            else:
                put(out, 3 * (w - 1) + k, new[k])
    energy = None
    for w in range(2, planes):
        h = field(get_a, weight, 1, even, w)
        new = heated(h, *trial_of(tb, w), beta)
        for k in range(3):
            put(out, 9 + 3 * (w - 2) + k, new[k])
        term = dot3(new, h)
        energy = term if energy is None else energy + term
    e_part[...] = energy
    out[pl.ds(EARLY * half, 8), :] = info[...].astype(F32)


def heat_late(planes, half, u, *refs):
    info, betas, w_in, w_x, sx, rx, ta, tb, rdx, inner, e_part = refs[:11]
    if u == 0:
        out, e_out, halo = refs[11:]
    else:
        e_other, out, e_out, halo = refs[11:]
    even = parity(info, half)
    columns = info.shape[-1]
    beta = jnp.broadcast_to(betas[0:1, :], (half, columns))
    weight = weight_of(w_in, w_x)
    get_b = second_planes(planes, half, sx, None, rx, None)

    def get_a(w, k):
        if w < 0:
            return halo[k]
        return tile(out, k, half) if w == 0 else tile(inner, 3 * (w - 1) + k, half)

    for w in (-1, 0):
        h = field(get_b, weight, 0, even, w)
        draw = trial_of(ta, w) if w >= 0 else trial_sent(rdx, u, half)
        new = heated(h, *draw, beta)
        for k in range(3):
            if w < 0:
                halo[k] = new[k]
            else:
                put(out, k, new[k])
    energy = e_part[...]
    for w in (0, 1):
        h = field(get_a, weight, 1, even, w)
        new = heated(h, *trial_of(tb, w), beta)
        for k in range(3):
            put(out, 3 + 3 * w + k, new[k])
        energy = energy + dot3(new, h)
    mine = jnp.full(e_out.shape, -jnp.sum(energy), F32)
    if u == 1:
        lane = lax.broadcasted_iota(jnp.int32, e_out.shape, 1)
        other = jnp.broadcast_to(e_other[0:1, : e_out.shape[1]], e_out.shape)
        mine = jnp.where(lane == 0, other, mine)
    e_out[...] = mine


def total_kernel(sites, parts, total):
    total[...] = jnp.sum(parts[...], axis=0, keepdims=True) / sites


def exchanged(u, info, note):
    place = lax.axis_index("temp")
    upper = slot_of(u) == 1
    ours = jnp.max(info[1:2, :]) > 0
    theirs = jnp.max(note[1:2, :]) > 0.5
    inside = jnp.where(upper, place != lax.axis_size("temp") - 1, place != 0)
    return jnp.logical_and(jnp.where(upper, ours, theirs), inside)


def out_kernel(planes, half, *refs):
    info0, info1, i0, i1, o0, o1, ri0, ri1, ro0, ro1, out_h, taken, out, sems = refs
    core = core_index()
    columns = out.shape[-1]
    pushes = []
    for u, info, own, other in ((0, info0, (i0, o0), (ri0, ro0)), (1, info1, (i1, o1), (ri1, ro1))):
        note = ri0[pl.ds(EARLY * half, 8), :] if u == 0 else ri1[pl.ds(EARLY * half, 8), :]
        take = exchanged(u, info, note)
        taken[u : u + 1, :] = jnp.full((1, columns), take.astype(jnp.int32), jnp.int32)

        def write(early, late, parities):
            even = (lax.broadcasted_iota(jnp.int32, (half, columns), 1) & 1) == jnp.broadcast_to(
                parities, (half, columns)
            )
            for w in range(planes):
                z = w + core * (planes - 1 - 2 * w)
                m = at_plane(even, w)
                for k in range(3):
                    a = tile(late, k, half) if w == 0 else tile(early, 3 * (w - 1) + k, half)
                    b = tile(late, 3 + 3 * w + k, half) if w < 2 else tile(early, 3 + 3 * w + k, half)
                    out[u, k, z, pl.ds(0, half, stride=2), :] = jnp.where(m, a, b)
                    out[u, k, z, pl.ds(1, half, stride=2), :] = jnp.where(m, b, a)

        @pl.when(take)
        def _():
            write(*other, note[0:1, :].astype(jnp.int32))

        @pl.when(jnp.logical_not(take))
        def _():
            write(*own, info[0:1, :])

        push = pltpu.make_async_copy(out.at[u], out_h.at[slot_of(u)], sems.at[u])
        push.start()
        pushes.append(push)
    for push in pushes:
        push.wait()


def energy_kernel(taken, total, r0, r1, energies_h, energies, sem):
    final = [
        jnp.where(taken[u : u + 1, u : u + 1] > 0, r[:, u : u + 1], total[:, u : u + 1])
        for u, r in ((0, r0), (1, r1))
    ]
    lane = lax.broadcasted_iota(jnp.int32, energies.shape, 1)
    energies[...] = jnp.where(
        lane == slot_of(0),
        jnp.broadcast_to(final[0], energies.shape),
        jnp.broadcast_to(final[1], energies.shape),
    )
    copy = pltpu.make_async_copy(energies, energies_h, sem)
    copy.start()
    copy.wait()


def step(
    spin_state, couplings, inverse_temps, colour_order, heat_level, heat_height, heat_angle, swap_bits
):
    replicas, _, planes, rows, columns = spin_state.shape
    half = rows // 2
    count = lax.axis_size("gz")
    temps = lax.axis_size("temp")
    assert replicas == 2 and planes == 4 and rows % 2 == 0 and columns % 2 == 0
    assert count % 2 == 0 and temps % 2 == 0
    in_chip = [(i, i ^ 1) for i in range(count)]
    cross = [(i, (i + (1 if i % 2 else -1)) % count) for i in range(count)]
    partners = (
        [(i, i ^ 1) for i in range(temps)],
        [(i, j) for i in range(temps) if 0 <= (j := i + (1 if i % 2 else -1)) < temps],
    )

    def swap_in(value):
        return lax.ppermute(value, "gz", in_chip)

    def swap_cross(value):
        return lax.ppermute(value, "gz", cross)

    def away(value, u):
        return lax.ppermute(value, "temp", partners[u])

    spins = PIECES * half
    pair = vm(6 * half, columns)
    p0x, p1x, pi, am0, am1, info0, info1, beta0, beta1 = kernel_call(
        functools.partial(load_kernel, planes, half),
        [vm(spins + 4 * rows, columns), vm(spins, columns), vm(2 * spins + 4 * rows, columns)]
        + [pair] * 2
        + [vm(8, columns, dtype=jnp.int32)] * 2
        + [vm(8, columns)] * 2,
        [HBM] * 5,
        scratch=[
            pltpu.SMEM((replicas,), jnp.int32),
            pltpu.SMEM((replicas,), jnp.int32),
            pltpu.SMEM((replicas,), F32),
            vm(planes, replicas, 3, rows, columns),
            pltpu.SemaphoreType.DMA((3 + planes,)),
            pltpu.SemaphoreType.DMA((2, 4)),
        ],
    )(*(in_hbm(v) for v in (swap_bits, colour_order, inverse_temps, spin_state, couplings)))
    info, beta = [info0, info1], [beta0, beta1]
    sx, si, a_in, a_x = [p0x, p1x], [pi, pi], [am0, am1], [[], []]
    rx = [swap_cross(sx[u]) for u in range(2)]
    ri = swap_in(pi)

    ta0, tb0, ta1, tb1, dx, di = kernel_call(
        functools.partial(trial_kernel, planes, half),
        [vm(planes, 4, half, columns)] * 4 + [pair] * 2,
        [SM, SM, VM, VM, VM],
    )(swap_bits, colour_order, heat_level, heat_height, heat_angle)
    trial_a, trial_b = [ta0, ta1], [tb0, tb1]
    rdx, rdi = swap_cross(dx), swap_in(di)

    w_in = kernel_call(
        functools.partial(weight_kernel, planes, half, True),
        [vm(2, planes, 6, half, columns)] * 2,
        [VM] * 4,
    )(couplings, ri, info0, info1)
    w_x = kernel_call(
        functools.partial(weight_kernel, planes, half, False),
        [vm(2, 2, 6, half, columns)] * 2,
        [VM] * 4,
    )(couplings, rx[0], info0, info1)

    assert OR_SWEEPS == 2
    for sweep in range(OR_SWEEPS):
        first = sweep == 0
        new_in, bi = [None] * 2, [None] * 2
        for u in range(2):
            new_in[u], bi[u] = kernel_call(
                functools.partial(relax_early, planes, half, first, u),
                [vm(3 * planes * half, columns), vm(6 * (1 + u) * half, columns)],
                [VM] * (6 + u),
            )(info[u], w_in[u], sx[u], si[u], ri, a_in[u], *bi[:u])
        for u in range(2):
            *a_x[u], sx[u] = kernel_call(
                functools.partial(relax_late, planes, half, first),
                [pair] * (1 + first),
                [VM] * (6 if first else 7),
                scratch=[] if first else [pair],
            )(info[u], w_in[u], w_x[u], sx[u], rx[u], new_in[u], *a_x[u])
            si[u], a_in[u] = bi[u], new_in[u]
            rx[u] = swap_cross(sx[u])
        ri = swap_in(bi[1])

    inner, outer, part, r_inner, r_outer = ([None] * 2 for _ in range(5))
    for u in range(2):
        inner[u], part[u] = kernel_call(
            functools.partial(heat_early, planes, half, u),
            [vm(EARLY * half + 8, columns), vm(half, columns)],
            [VM] * 9,
            scratch=[vm(3, half, columns)],
        )(info[u], beta[u], w_in[u], sx[u], si[u], ri, trial_a[u], trial_b[u], rdi)
        r_inner[u] = away(inner[u], u)
    energy = []
    for u in range(2):
        outer[u], *energy = kernel_call(
            functools.partial(heat_late, planes, half, u),
            [vm(LATE * half, columns), vm(count, 2) if u else vm(8, columns)],
            [VM] * (11 + u),
            scratch=[vm(3, half, columns)],
        )(
            info[u], beta[u], w_in[u], w_x[u], sx[u], rx[u],
            trial_a[u], trial_b[u], rdx, inner[u], part[u], *energy,
        )
        r_outer[u] = away(outer[u], u)

    parts = lax.all_to_all(energy[0], "gz", split_axis=0, concat_axis=0, tiled=True)
    (total,) = kernel_call(
        functools.partial(total_kernel, float(columns * rows * planes * count)), [vm(1, 2)], [VM]
    )(parts)
    r_total = [away(total, u) for u in range(2)]

    spin_final, taken = kernel_call(
        functools.partial(out_kernel, planes, half),
        [jax.ShapeDtypeStruct(spin_state.shape, F32), vm(8, columns, dtype=jnp.int32)],
        [VM] * 10,
        out_specs=[HBM, VM],
        scratch=[vm(*spin_state.shape), pltpu.SemaphoreType.DMA((2,))],
    )(info0, info1, *inner, *outer, *r_inner, *r_outer)
    (energies,) = kernel_call(
        energy_kernel,
        [jax.ShapeDtypeStruct((1, 2), F32)],
        [VM] * 4,
        out_specs=[HBM],
        scratch=[vm(1, 2), pltpu.SemaphoreType.DMA(())],
    )(taken, total, *r_total)
    return spin_final, energies.reshape(-1)


def solution(mesh):
    return jax.shard_map(
        step,
        mesh=mesh,
        in_specs=(
            P(("group", "temp"), None, "gz", None, None),
            P(None, ("group", "gz"), None, None),
            P(("group", "temp")),
            P(("group", "temp")),
            P(("group", "temp"), "gz", None, None),
            P(("group", "temp"), "gz", None, None),
            P(("group", "temp"), "gz", None, None),
            P(("group", "temp")),
        ),
        out_specs=(P(("group", "temp"), None, "gz", None, None), P(("group", "temp"))),
        check_vma=False,
    )
```
